32 devices in a mesh: dp: 2 (over x), ep: 16 (over z, y, core).
Axes of the slice: x: 2, y: 2, z: 4, core: 2. Of those that a mesh axis runs over, the one named last changes fastest.
Arguments:
- x_in: bfloat16 [1024, 2048], P(('dp', 'ep')), parts along dimension 0
- expert_ids: int32 [1024, 8], P(('dp', 'ep')), parts along dimension 0
- norm_weight: bfloat16 [2048], replicated
- router_w: bfloat16 [2048, 64], replicated
- router_b: bfloat16 [64], replicated
- w_gate_up: bfloat16 [64, 2048, 2048], P('ep')
- b_gate_up: bfloat16 [64, 2048], P('ep')
- w_down: bfloat16 [64, 1024, 2048], P('ep')
- b_down: bfloat16 [64, 2048], P('ep')
Outputs:
- output: bfloat16 [1024, 2048], P(('dp', 'ep')), parts along dimension 0
There are 2 independent parts. The reference program is written for one: setup_inputs(seed, part) draws one part's arguments, and reference() takes and returns one part's arrays. A program takes and returns all parts, laid end to end along the dimension named above; an argument that names none is the same for every part.
All inputs are finite; a program needn't handle non-finite values.
Results may differ from the reference program's by a relative error of at most 0.0063795.
Values are sent between devices in bfloat16 or wider.
A program may use at most 1 GiB of HBM per device.

```python
import jax
import jax.numpy as jnp
from jax import lax

D_MODEL = 2048
D_FF = 1024
EXPERTS = 64
TOP_K = 8
TOK_DEV = 32
GROUP_SIZE = 16

TOKENS = TOK_DEV * GROUP_SIZE
CAPACITY = 4 * TOP_K * TOK_DEV // EXPERTS
HOT_COUNT = EXPERTS // 8
EPSILON = 1e-5
LIMIT = 7.0
ALPHA = 1.702


def draw_routes(key):
    key_hot, key_src = jax.random.split(key)
    expert_order = jax.random.permutation(key_hot, EXPERTS)
    cold_total = TOP_K * TOK_DEV - HOT_COUNT * CAPACITY
    cold_count = EXPERTS - HOT_COUNT
    position = jnp.arange(EXPERTS)
    extra = (position - HOT_COUNT < cold_total % cold_count).astype(jnp.int32)
    counts = jnp.where(position < HOT_COUNT, CAPACITY, cold_total // cold_count + extra)
    ends = jnp.cumsum(counts)
    slot_rank = jnp.sum(jnp.arange(TOP_K * TOK_DEV)[:, None] >= ends[None, :], axis=1)

    def one_source(src_key):
        key_cold, key_tok = jax.random.split(src_key)
        cold = jax.random.permutation(key_cold, expert_order[HOT_COUNT:])
        order = jnp.concatenate([expert_order[:HOT_COUNT], cold])
        table = order[slot_rank].reshape(TOP_K, TOK_DEV).T
        return table[jax.random.permutation(key_tok, TOK_DEV)]

    tables = jax.vmap(one_source)(jax.random.split(key_src, GROUP_SIZE))
    return tables.reshape(TOKENS, TOP_K).astype(jnp.int32)


def stacked_normal(key, shape, scale):
    def one_expert(expert_key):
        return (jax.random.normal(expert_key, shape, jnp.float32) * scale).astype(jnp.bfloat16)
    return lax.map(one_expert, jax.random.split(key, EXPERTS))


def setup_inputs(seed: int = 0, part: int = 0) -> dict:
    shared = jax.random.split(jax.random.key(seed), 7)
    own = jax.random.split(jax.random.fold_in(jax.random.key(seed + 1), part), 2)
    x_in = jax.random.normal(own[0], (TOKENS, D_MODEL), jnp.float32).astype(jnp.bfloat16)
    expert_ids = draw_routes(own[1])
    norm_weight = (1.0 + 0.3 * jax.random.normal(shared[0], (D_MODEL,), jnp.float32)).astype(jnp.bfloat16)
    router_w = (jax.random.normal(shared[1], (D_MODEL, EXPERTS), jnp.float32) * D_MODEL ** -0.5).astype(jnp.bfloat16)
    router_b = (0.7 * jax.random.normal(shared[2], (EXPERTS,), jnp.float32)).astype(jnp.bfloat16)
    w_gate_up = stacked_normal(shared[3], (D_MODEL, 2 * D_FF), 5.0 * D_MODEL ** -0.5)
    b_gate_up = jax.random.normal(shared[4], (EXPERTS, 2 * D_FF), jnp.float32).astype(jnp.bfloat16)
    w_down = stacked_normal(shared[5], (D_FF, D_MODEL), 0.125 * D_FF ** -0.5)
    b_down = (0.5 * jax.random.normal(shared[6], (EXPERTS, D_MODEL), jnp.float32)).astype(jnp.bfloat16)
    return dict(x_in=x_in, expert_ids=expert_ids, norm_weight=norm_weight, router_w=router_w, router_b=router_b, w_gate_up=w_gate_up, b_gate_up=b_gate_up, w_down=w_down, b_down=b_down)


def clamped_glu(gate_up):
    gate = jnp.minimum(gate_up[..., 0::2].astype(jnp.float32), LIMIT)
    linear = jnp.clip(gate_up[..., 1::2].astype(jnp.float32), -LIMIT, LIMIT)
    return (gate * jax.nn.sigmoid(ALPHA * gate) * (linear + 1.0)).astype(jnp.bfloat16)


def reference(x_in, expert_ids, norm_weight, router_w, router_b, w_gate_up, b_gate_up, w_down, b_down):
    x_float = x_in.astype(jnp.float32)
    inv_rms = lax.rsqrt(jnp.mean(x_float * x_float, axis=-1, keepdims=True) + EPSILON)
    hidden = (x_float * inv_rms * norm_weight.astype(jnp.float32)).astype(jnp.bfloat16)
    logits = jnp.dot(hidden, router_w, preferred_element_type=jnp.float32) + router_b.astype(jnp.float32)
    gates = jax.nn.softmax(jnp.take_along_axis(logits, expert_ids, axis=1), axis=-1)
    flat_ids = expert_ids.reshape(-1)
    flat_gates = gates.reshape(-1)
    max_rows = GROUP_SIZE * CAPACITY

    def one_expert(combined, weights):
        expert, gate_up_w, gate_up_b, down_w, down_b = weights
        chosen = flat_ids == expert
        picks = jnp.nonzero(chosen, size=max_rows, fill_value=0)[0]
        valid = jnp.arange(max_rows) < jnp.sum(chosen)
        row_token = picks // TOP_K
        rows = hidden[row_token]
        gate_up = (jnp.dot(rows, gate_up_w, preferred_element_type=jnp.float32) + gate_up_b.astype(jnp.float32)).astype(jnp.bfloat16)
        glu_out = clamped_glu(gate_up)
        expert_out = (jnp.dot(glu_out, down_w, preferred_element_type=jnp.float32) + down_b.astype(jnp.float32)).astype(jnp.bfloat16)
        scale = jnp.where(valid, flat_gates[picks], 0.0)
        combined = combined.at[row_token].add(scale[:, None] * expert_out.astype(jnp.float32))
        return combined, None

    start_sum = jnp.zeros((TOKENS, D_MODEL), jnp.float32)
    combined, _ = lax.scan(one_expert, start_sum, (jnp.arange(EXPERTS, dtype=jnp.int32), w_gate_up, b_gate_up, w_down, b_down))
    return (x_float + combined).astype(jnp.bfloat16)
```

```python
import jax
import jax.numpy as jnp
from jax import lax
from jax.sharding import PartitionSpec as P

CAPACITY_FACTOR = 4
EPSILON = 1e-5
LIMIT = 7.0
ALPHA = 1.702


def rms_norm(x_in, norm_weight):
    x_float = x_in.astype(jnp.float32)
    inv_rms = lax.rsqrt(jnp.mean(x_float * x_float, axis=-1, keepdims=True) + EPSILON)
    return (x_float * inv_rms * norm_weight.astype(jnp.float32)).astype(jnp.bfloat16)


def dense_gates(hidden, expert_ids, router_w, router_b):
    logits = jnp.dot(hidden, router_w, preferred_element_type=jnp.float32) + router_b.astype(jnp.float32)
    experts = router_w.shape[1]
    chosen = jnp.any(expert_ids[:, :, None] == jnp.arange(experts, dtype=jnp.int32)[None, None, :], axis=1)
    top = jnp.max(jnp.where(chosen, logits, -jnp.inf), axis=-1, keepdims=True)
    weight = jnp.where(chosen, jnp.exp(logits - top), 0.0)
    return jnp.where(chosen, weight / jnp.sum(weight, axis=-1, keepdims=True), -1.0)


def solution(mesh):
    n_group = mesh.shape['ep']
    rows_spec = P(('dp', 'ep'), None)

    def local_block(x_in, expert_ids, norm_weight, router_w, router_b, w_gate_up, b_gate_up, w_down, b_down):
        tok_dev, d_model = x_in.shape
        top_k = expert_ids.shape[1]
        local_exp = w_gate_up.shape[0]
        experts = local_exp * n_group
        d_ff = w_down.shape[1]
        capacity = CAPACITY_FACTOR * top_k * tok_dev // experts
        hidden = rms_norm(x_in, norm_weight)
        gates = dense_gates(hidden, expert_ids, router_w, router_b)
        tokens = n_group * tok_dev
        slots = n_group * capacity
        h_all = lax.all_gather(hidden, 'ep', axis=0, tiled=True)
        g_all = lax.all_gather(gates, 'ep', axis=0, tiled=True)
        g_loc = lax.dynamic_slice(g_all, (0, lax.axis_index('ep') * local_exp), (tokens, local_exp))
        mask = (g_loc >= 0).reshape(n_group, tok_dev, local_exp)
        rank = jnp.cumsum(mask.astype(jnp.int32), axis=1) - 1
        slot = rank + (jnp.arange(n_group, dtype=jnp.int32) * capacity)[:, None, None]
        slot = jnp.where(mask, slot, -1).reshape(tokens, local_exp).T
        onehot = (slot[:, None, :] == jnp.arange(slots, dtype=jnp.int32)[None, :, None]).astype(jnp.bfloat16)
        rows = jnp.einsum('est,td->esd', onehot, h_all, preferred_element_type=jnp.float32).astype(jnp.bfloat16)
        u = (jnp.einsum('esd,edf->esf', rows, w_gate_up, preferred_element_type=jnp.float32) + b_gate_up[:, None, :].astype(jnp.float32)).astype(jnp.bfloat16)
        i = jnp.arange(256)
        perm = ((i[:, None] // 2 + 128 * (i[:, None] % 2)) == i[None, :]).astype(jnp.bfloat16)
        v = jnp.einsum('esbi,ij->esbj', u.reshape(local_exp, slots, -1, 256), perm, preferred_element_type=jnp.float32)
        a = jnp.minimum(v[..., :128], LIMIT)
        l = jnp.clip(v[..., 128:], -LIMIT, LIMIT)
        z = (a * jax.nn.sigmoid(ALPHA * a) * (l + 1.0)).astype(jnp.bfloat16).reshape(local_exp, slots, d_ff)
        y = (jnp.einsum('esf,efd->esd', z, w_down, preferred_element_type=jnp.float32) + b_down[:, None, :].astype(jnp.float32)).astype(jnp.bfloat16)
        back = jnp.einsum('est,esd->etd', onehot, y, preferred_element_type=jnp.float32)
        part = jnp.sum(jnp.maximum(g_loc, 0.0).T[:, :, None] * back, axis=0)
        mixed = lax.psum_scatter(part, 'ep', scatter_dimension=0, tiled=True)
        return (x_in.astype(jnp.float32) + mixed).astype(jnp.bfloat16)

    return jax.shard_map(local_block, mesh=mesh, in_specs=(rows_spec, rows_spec, P(), P(), P(), P('ep', None, None), P('ep', None), P('ep', None, None), P('ep', None)), out_specs=rows_spec, check_vma=False)
```

```python
import functools

import jax
import jax.numpy as jnp
from jax import lax
from jax.experimental import pallas as pl
from jax.experimental.pallas import tpu as pltpu
from jax.sharding import PartitionSpec as P

CAPACITY_FACTOR = 4
EPSILON = 1e-5
LIMIT = 7.0
ALPHA = 1.702
MESH = pl.DeviceIdType.MESH
PIECES = 4
F32 = jnp.float32
BF16 = jnp.bfloat16


def dot(a, b):
    return jnp.dot(a, b, preferred_element_type=F32)


def iota(shape, dim):
    return lax.broadcasted_iota(jnp.int32, shape, dim)


def moe_kernel(cfg, x_ref, ids_ref, g_ref, wr_ref, br_ref, wgu_hbm, bgu_ref, wd_hbm, bd_ref, out_ref,
               wgu, wd, hid, gate, sel, back, pgate, slot_t, rows, glu, perm, bgu, bd,
               acc, r_core, r_y, r_near, r_mid, r_far,
               s_w, s_h, q_h, s_g, q_g, s_core, q_core, s_y, q_y, s_near, q_near, s_mid, q_mid, s_far, q_far, s_fwd):
    tok, d_model, d_ff, top_k, experts, local_exp, cap = cfg
    tc = 8 * tok
    ns = 8 * cap
    cw = d_model // PIECES
    me = lax.axis_index('ep')
    z, y, c = lax.div(me, 4), lax.rem(lax.div(me, 2), 2), lax.rem(me, 2)
    pair, zin = lax.div(z, 2), lax.rem(z, 2)
    is_mid = zin != pair
    is_end = zin == pair
    partner, ypeer, zpeer, midpeer = me + 1 - 2 * c, me + 2 - 4 * y, me + 4 - 8 * zin, me + 4 - 8 * pair

    def pos(q, cc, yy, zz):
        return ((q * 2 + cc) * 2 + yy) * 2 + zz

    def remote(src, dst, send, recv, dev):
        return pltpu.make_async_remote_copy(src_ref=src, dst_ref=dst, send_sem=send, recv_sem=recv,
                                            device_id={'ep': dev}, device_id_type=MESH)

    def w_copy(i):
        if i < local_exp:
            return pltpu.make_async_copy(wgu_hbm.at[i], wgu.at[i], s_w.at[i])
        return pltpu.make_async_copy(wd_hbm.at[i - local_exp], wd.at[i - local_exp], s_w.at[i])

    for i in range(2 * local_exp):
        w_copy(i).start()

    barrier = pltpu.get_barrier_semaphore()
    for dev in (partner, ypeer, zpeer):
        pl.semaphore_signal(barrier, inc=1, device_id={'ep': dev}, device_id_type=MESH)

    @pl.when(is_mid)
    def _():
        pl.semaphore_signal(barrier, inc=1, device_id={'ep': midpeer}, device_id_type=MESH)

    own = pos(pair, c, y, zin)
    x = x_ref[...].astype(F32)
    inv = lax.rsqrt(jnp.mean(x * x, axis=-1, keepdims=True) + EPSILON)
    h = (x * inv * g_ref[...].astype(F32)).astype(BF16)
    hid[pl.ds(own * tok, tok), :] = h
    logits = dot(h, wr_ref[...]) + br_ref[...].astype(F32)
    lane_e = iota((tok, experts), 1)
    ids = ids_ref[...]
    chosen = ids[:, 0:1] == lane_e
    for k in range(1, top_k):
        chosen = jnp.logical_or(chosen, ids[:, k:k + 1] == lane_e)
    top = jnp.max(jnp.where(chosen, logits, -jnp.inf), axis=-1, keepdims=True)
    weight = jnp.where(chosen, jnp.exp(jnp.where(chosen, logits - top, 0.0)), 0.0)
    gates = jnp.where(chosen, weight / jnp.sum(weight, axis=-1, keepdims=True), -1.0)
    gate[pl.ds(own * tok, tok), :] = jnp.concatenate([gates, jnp.full((tok, 128 - experts), -1.0, F32)], axis=1)

    @pl.when(is_mid)
    def _():
        pl.semaphore_wait(barrier, 4)

    @pl.when(is_end)
    def _():
        pl.semaphore_wait(barrier, 3)

    def block(b, d, dev):
        rs = pl.ds(b * tok, tok)
        return (remote(hid.at[rs], hid.at[rs], s_h.at[d, b], q_h.at[b], dev),
                remote(gate.at[rs], gate.at[rs], s_g.at[d, b], q_g.at[b], dev))

    TO_Z, TO_Y, TO_C, TO_M = 0, 1, 2, 3
    dest = {TO_Z: zpeer, TO_Y: ypeer, TO_C: partner, TO_M: midpeer}

    def send(b, *ds):
        for d in ds:
            for cp in block(b, d, dest[d]):
                cp.start()

    def sent(b, *ds):
        for d in ds:
            for cp in block(b, d, dest[d]):
                cp.wait_send()

    def arrived(b):
        for cp in block(b, 0, zpeer):
            cp.wait_recv()

    near = pos(pair, c, y, 1 - zin)
    y_own, y_near = pos(pair, c, 1 - y, zin), pos(pair, c, 1 - y, 1 - zin)
    far = [pos(1 - pair, c, y, pair), pos(1 - pair, c, y, 1 - pair)]
    y_far = [pos(1 - pair, c, 1 - y, pair), pos(1 - pair, c, 1 - y, 1 - pair)]

    send(own, TO_Z, TO_Y)

    @pl.when(is_mid)
    def _():
        send(own, TO_M)
    send(own, TO_C)

    bgu[...] = bgu_ref[...].astype(F32)
    bd[...] = bd_ref[...].astype(F32)
    pi, pj = iota((256, 256), 0), iota((256, 256), 1)
    perm[...] = (lax.div(pi, 2) + 128 * lax.rem(pi, 2) == pj).astype(F32).astype(BF16)

    arrived(y_own)
    send(y_own, TO_C)
    arrived(near)
    send(near, TO_Y)

    @pl.when(is_mid)
    def _():
        send(near, TO_M)
    send(near, TO_C)
    arrived(y_near)
    send(y_near, TO_C)
    for yy in range(2):
        for zz in range(2):
            arrived(pos(pair, 1 - c, yy, zz))

    def forward_far():
        @pl.when(is_mid)
        def _():
            for b in far:
                arrived(b)
                send(b, TO_Z, TO_Y)
                send(b, TO_C)

    def forward_far_end():
        @pl.when(is_end)
        def _():
            for b in far:
                arrived(b)
                send(b, TO_Y)
                send(b, TO_C)

    def forward_far_y():
        for b in y_far:
            arrived(b)
            send(b, TO_C)

    def finish_far():
        for yy in range(2):
            for zz in range(2):
                arrived(pos(1 - pair, 1 - c, yy, zz))

    def route(q):
        g = gate[pl.ds(q * tc, tc), :]
        hit = g >= 0.0
        ri, rj = iota((tc, tc), 0), iota((tc, tc), 1)
        before = jnp.logical_and(rj < ri, lax.div(rj, tok) == lax.div(ri, tok)).astype(F32).astype(BF16)
        rank = dot(before, hit.astype(F32).astype(BF16))
        base = (lax.div(iota((tc, 128), 0), tok) * cap).astype(F32)
        slot = jnp.where(hit, rank + base, -1.0)
        slot_t[...] = slot.T
        lane = iota((tc, 128), 1)
        s_lane = iota((tc, ns), 1).astype(F32)
        s_row = iota((ns, tc), 0).astype(F32)
        for e in range(local_exp):
            col = me * local_exp + e
            pick = lane == col
            p_e = jnp.sum(jnp.where(pick, jnp.maximum(g, 0.0), 0.0), axis=1, keepdims=True)
            s_e = jnp.sum(jnp.where(pick, slot, 0.0), axis=1, keepdims=True)
            back[:, e * ns:(e + 1) * ns] = (s_e == s_lane).astype(F32).astype(BF16)
            pgate[:, e * 128:(e + 1) * 128] = jnp.broadcast_to(p_e, (tc, 128))
            sel[e * ns:(e + 1) * ns, :] = (slot_t[pl.ds(col, 1), :] == s_row).astype(F32).astype(BF16)

    nb_w = 512
    def gate_up(e, q):
        pick = sel[pl.ds(e * ns, ns), :]
        valid = jnp.max(pick.astype(F32), axis=1, keepdims=True) > 0.0
        for i in range(d_model // nb_w):
            sl = slice(i * nb_w, (i + 1) * nb_w)
            rows[:, sl] = dot(pick, hid[pl.ds(q * tc, tc), sl]).astype(BF16)
        for i in range(2 * d_ff // nb_w):
            sl = slice(i * nb_w, (i + 1) * nb_w)
            u = (dot(rows[...], wgu[e, :, sl]) + bgu[pl.ds(e, 1), sl]).astype(BF16)
            for j in range(nb_w // 256):
                v = dot(u[:, j * 256:(j + 1) * 256], perm[...])
                a = jnp.minimum(v[:, :128], LIMIT)
                l = jnp.clip(v[:, 128:], -LIMIT, LIMIT)
                o = a * jax.nn.sigmoid(ALPHA * a) * (l + 1.0)
                m = i * (nb_w // 256) + j
                glu[e, :, m * 128:(m + 1) * 128] = jnp.where(valid, o, 0.0).astype(BF16)

    def down(n, k):
        cols = pl.ds(pl.multiple_of(n * cw, 128), cw)
        for e in range(local_exp):
            y_e = (dot(glu[e], wd[e, :, cols]) + bd[e:e + 1, cols]).astype(BF16)
            t = dot(back[:, e * ns:(e + 1) * ns], y_e)
            p_e = pgate[:, e * 128:(e + 1) * 128]
            for j in range(cw // 128):
                js = slice(j * 128, (j + 1) * 128)
                if e == 0:
                    acc[k, n, :, js] = p_e * t[:, js]
                else:
                    acc[k, n, :, js] += p_e * t[:, js]

    def core_copy(k, n):
        return remote(acc.at[k, n, pl.ds((1 - c) * 4 * tok, 4 * tok)], r_core.at[k, n], s_core.at[k, n], q_core.at[k, n], partner)

    def y_copy(k, n):
        return remote(acc.at[k, n, pl.ds((c * 2 + 1 - y) * 2 * tok, 2 * tok)], r_y.at[k, n], s_y.at[k, n], q_y.at[k, n], ypeer)

    mine = (c * 2 + y) * 2 * tok

    def near_copy(n):
        return remote(acc.at[0, n, pl.ds(mine + (1 - zin) * tok, tok)], r_near.at[n], s_near.at[n], q_near.at[n], zpeer)

    def mid_copy(n):
        return remote(acc.at[1, n, pl.ds(mine, 2 * tok)], r_mid.at[n], s_mid.at[n], q_mid.at[n], zpeer)

    def far_copy(n):
        return remote(acc.at[1, n, pl.ds(mine, 2 * tok)], r_far.at[n], s_far.at[n], q_far.at[n], midpeer)

    def fwd_copy(n):
        return remote(r_far.at[n, pl.ds((1 - zin) * tok, tok)], r_far.at[n, pl.ds(0, tok)], s_fwd.at[n], q_far.at[n], zpeer)

    def after_core(k, n):
        core_copy(k, n).wait_recv()
        other = pl.ds((1 - y) * 2 * tok, 2 * tok)
        acc[k, n, pl.ds((c * 2 + 1 - y) * 2 * tok, 2 * tok)] += r_core[k, n, other]
        y_copy(k, n).start()
        acc[k, n, pl.ds(mine, 2 * tok)] += r_core[k, n, pl.ds(y * 2 * tok, 2 * tok)]

    def after_y(k, n):
        y_copy(k, n).wait_recv()
        acc[k, n, pl.ds(mine, 2 * tok)] += r_y[k, n]
        if k == 0:
            near_copy(n).start()
        else:
            @pl.when(is_end)
            def _():
                mid_copy(n).start()

    def at_mid(n):
        @pl.when(is_mid)
        def _():
            mid_copy(n).wait_recv()
            acc[1, n, pl.ds(mine, 2 * tok)] += r_mid[n]
            far_copy(n).start()

    def forward(n):
        @pl.when(is_mid)
        def _():
            far_copy(n).wait_recv()
            fwd_copy(n).start()

    def finish(n):
        @pl.when(is_end)
        def _():
            fwd_copy(n).wait_recv()
        near_copy(n).wait_recv()
        cols = slice(n * cw, (n + 1) * cw)
        total = acc[0, n, pl.ds(mine + zin * tok, tok)] + r_near[n]
        total = total + r_far[n, pl.ds(jnp.where(is_mid, zin, 0) * tok, tok)]
        out_ref[:, cols] = (x_ref[:, cols].astype(F32) + total).astype(BF16)

    forward_far()
    route(pair)

    def up0(e, _):
        for i in range(local_exp):
            @pl.when(e == i)
            def _():
                w_copy(i).wait()
        gate_up(e, pair)

        @pl.when(e == 1)
        def _():
            forward_far_end()

        @pl.when(e == 3)
        def _():
            forward_far_y()
        return 0
    lax.fori_loop(0, local_exp, up0, 0)
    for i in range(local_exp, 2 * local_exp):
        w_copy(i).wait()

    def down0(n, _):
        down(n, 0)
        core_copy(0, n).start()

        @pl.when(n > 0)
        def _():
            after_core(0, n - 1)
        return 0
    lax.fori_loop(0, PIECES, down0, 0)

    finish_far()
    route(1 - pair)
    after_core(0, PIECES - 1)

    def up1(e, _):
        gate_up(e, 1 - pair)
        after_y(0, e)
        return 0
    lax.fori_loop(0, local_exp, up1, 0)

    def down1(n, _):
        down(n, 1)
        core_copy(1, n).start()

        @pl.when(n > 0)
        def _():
            after_core(1, n - 1)
        return 0
    lax.fori_loop(0, PIECES, down1, 0)
    after_core(1, PIECES - 1)
    for n in range(PIECES):
        after_y(1, n)
        at_mid(n)
        if n > 0:
            forward(n - 1)
    forward(PIECES - 1)
    for n in range(PIECES):
        finish(n)

    sent(own, TO_Z, TO_Y, TO_C)
    sent(near, TO_Y, TO_C)
    sent(y_own, TO_C)
    sent(y_near, TO_C)
    for b in far:
        sent(b, TO_Y, TO_C)
    for b in y_far:
        sent(b, TO_C)
    for n in range(PIECES):
        for k in range(2):
            core_copy(k, n).wait_send()
            y_copy(k, n).wait_send()
        near_copy(n).wait_send()

    @pl.when(is_mid)
    def _():
        sent(own, TO_M)
        sent(near, TO_M)
        for b in far:
            sent(b, TO_Z)
        for n in range(PIECES):
            far_copy(n).wait_send()
            fwd_copy(n).wait_send()

    @pl.when(is_end)
    def _():
        for n in range(PIECES):
            mid_copy(n).wait_send()


def solution(mesh):
    n_group = mesh.shape['ep']
    rows_spec = P(('dp', 'ep'), None)

    def local_block(x_in, expert_ids, norm_weight, router_w, router_b, w_gate_up, b_gate_up, w_down, b_down):
        tok, d_model = x_in.shape
        top_k = expert_ids.shape[1]
        local_exp, d_ff = w_down.shape[0], w_down.shape[1]
        experts = local_exp * n_group
        cap = CAPACITY_FACTOR * top_k * tok // experts
        cfg = (tok, d_model, d_ff, top_k, experts, local_exp, cap)
        tc, ns, cw = 8 * tok, 8 * cap, d_model // PIECES
        vm = pl.BlockSpec(memory_space=pltpu.VMEM)
        hbm = pl.BlockSpec(memory_space=pl.ANY)
        dma = pltpu.SemaphoreType.DMA
        return pl.pallas_call(
            functools.partial(moe_kernel, cfg),
            out_shape=jax.ShapeDtypeStruct((tok, d_model), BF16),
            in_specs=[vm, vm, vm, vm, vm, hbm, vm, hbm, vm],
            out_specs=vm,
            scratch_shapes=[
                pltpu.VMEM((local_exp, d_model, 2 * d_ff), BF16),
                pltpu.VMEM((local_exp, d_ff, d_model), BF16),
                pltpu.VMEM((n_group * tok, d_model), BF16),
                pltpu.VMEM((n_group * tok, 128), F32),
                pltpu.VMEM((local_exp * ns, tc), BF16),
                pltpu.VMEM((tc, local_exp * ns), BF16),
                pltpu.VMEM((tc, local_exp * 128), F32),
                pltpu.VMEM((128, tc), F32),
                pltpu.VMEM((ns, d_model), BF16),
                pltpu.VMEM((local_exp, ns, d_ff), BF16),
                pltpu.VMEM((256, 256), BF16),
                pltpu.VMEM((local_exp, 2 * d_ff), F32),
                pltpu.VMEM((local_exp, d_model), F32),
                pltpu.VMEM((2, PIECES, tc, cw), F32),
                pltpu.VMEM((2, PIECES, 4 * tok, cw), F32),
                pltpu.VMEM((2, PIECES, 2 * tok, cw), F32),
                pltpu.VMEM((PIECES, tok, cw), F32),
                pltpu.VMEM((PIECES, 2 * tok, cw), F32),
                pltpu.VMEM((PIECES, 2 * tok, cw), F32),
                dma((2 * local_exp,)),
                dma((4, n_group)), dma((n_group,)), dma((4, n_group)), dma((n_group,)),
                dma((2, PIECES)), dma((2, PIECES)), dma((2, PIECES)), dma((2, PIECES)),
                dma((PIECES,)), dma((PIECES,)), dma((PIECES,)), dma((PIECES,)),
                dma((PIECES,)), dma((PIECES,)), dma((PIECES,)),
            ],
            compiler_params=pltpu.CompilerParams(
                collective_id=0, has_side_effects=True, vmem_limit_bytes=67043328),
            name='moe_block',
        )(x_in, expert_ids, norm_weight.reshape(1, -1), router_w, router_b.reshape(1, -1), w_gate_up, b_gate_up, w_down, b_down)

    return jax.shard_map(local_block, mesh=mesh, in_specs=(rows_spec, rows_spec, P(), P(), P(), P('ep', None, None), P('ep', None), P('ep', None, None), P('ep', None)), out_specs=rows_spec, check_vma=False)
```

```python
import functools

import jax
import jax.numpy as jnp
from jax import lax
from jax.experimental import pallas as pl
from jax.experimental.pallas import tpu as pltpu
from jax.sharding import PartitionSpec as P

CAPACITY_FACTOR = 4
EPSILON = 1e-5
LIMIT = 7.0
ALPHA = 1.702
MESH = pl.DeviceIdType.MESH
PIECES = 8
STEPS = 4
F32 = jnp.float32
BF16 = jnp.bfloat16


def dot(a, b):
    return jnp.dot(a, b, preferred_element_type=F32)


def iota(shape, dim):
    return lax.broadcasted_iota(jnp.int32, shape, dim)


def moe_kernel(cfg, x_ref, ids_ref, g_ref, wr_ref, br_ref, wgu_hbm, bgu_ref, wd_hbm, bd_ref, out_ref,
               wgu, wd, hid, gate, sel, back, pgate, slot_t, rows, glu, perm, bgu, bd,
               acc, r_core, r_y, r_z,
               s_w, s_h, q_h, s_g, q_g, s_core, q_core, s_y, q_y, s_z, q_z):
    tok, d_model, d_ff, top_k, experts, local_exp, cap = cfg
    tc = 8 * tok
    ns = 8 * cap
    cw = d_model // PIECES
    half = tok // 2
    me = lax.axis_index('ep')
    z, y, c = lax.div(me, 4), lax.rem(lax.div(me, 2), 2), lax.rem(me, 2)
    pair, zin = lax.div(z, 2), lax.rem(z, 2)
    partner, ypeer, zpeer = me + 1 - 2 * c, me + 2 - 4 * y, me + 4 - 8 * zin
    zfar = [me + 4 * (2 * (1 - pair) + j - z) for j in range(2)]

    def pos(q, cc, yy, zz):
        return ((q * 2 + cc) * 2 + yy) * 2 + zz

    def remote(src, dst, send, recv, dev):
        return pltpu.make_async_remote_copy(src_ref=src, dst_ref=dst, send_sem=send, recv_sem=recv,
                                            device_id={'ep': dev}, device_id_type=MESH)

    def w_copy(i):
        if i < local_exp:
            return pltpu.make_async_copy(wgu_hbm.at[i], wgu.at[i], s_w.at[i])
        return pltpu.make_async_copy(wd_hbm.at[i - local_exp], wd.at[i - local_exp], s_w.at[i])

    for i in range(2 * local_exp):
        w_copy(i).start()

    barrier = pltpu.get_barrier_semaphore()
    for dev in (partner, ypeer, zpeer, *zfar):
        pl.semaphore_signal(barrier, inc=1, device_id={'ep': dev}, device_id_type=MESH)

    own = pos(pair, c, y, zin)
    x = x_ref[...].astype(F32)
    inv = lax.rsqrt(jnp.mean(x * x, axis=-1, keepdims=True) + EPSILON)
    h = (x * inv * g_ref[...].reshape(1, d_model).astype(F32)).astype(BF16)
    hid[pl.ds(own * tok, tok), :] = h
    pl.semaphore_wait(barrier, 5)

    TO_Z, TO_Y, TO_C, TO_F0, TO_F1 = range(5)
    dest = [zpeer, ypeer, partner, zfar[0], zfar[1]]

    def h_copy(b, d, s):
        rs = pl.ds(b * tok + s * half, half)
        return remote(hid.at[rs], hid.at[rs], s_h.at[d, b, s], q_h.at[b, s], dest[d])

    def g_copy(b, d):
        rs = pl.ds(b * tok, tok)
        return remote(gate.at[rs], gate.at[rs], s_g.at[d, b], q_g.at[b], dest[d])

    def send_h(b, s, *ds):
        for d in ds:
            h_copy(b, d, s).start()

    def send_g(b, *ds):
        for d in ds:
            g_copy(b, d).start()

    def pass_h(b, s, *ds):
        h_copy(b, 0, s).wait_recv()
        send_h(b, s, *ds)

    def pass_g(b, *ds):
        g_copy(b, 0).wait_recv()
        send_g(b, *ds)

    def sent(b, *ds):
        for d in ds:
            for s in range(2):
                h_copy(b, d, s).wait_send()
            g_copy(b, d).wait_send()

    near = pos(pair, c, y, 1 - zin)
    y_own, y_near = pos(pair, c, 1 - y, zin), pos(pair, c, 1 - y, 1 - zin)
    far = [pos(1 - pair, c, y, j) for j in range(2)]
    y_far = [pos(1 - pair, c, 1 - y, j) for j in range(2)]

    for s in range(2):
        send_h(own, s, TO_Z, TO_Y)
    for s in range(2):
        send_h(own, s, TO_C)

    logits = lax.dot_general(h, wr_ref[...], (((1,), (1,)), ((), ())), preferred_element_type=F32) + br_ref[...].astype(F32)
    lane_e = iota((tok, experts), 1)
    ids = ids_ref[...].T
    chosen = ids[:, 0:1] == lane_e
    for k in range(1, top_k):
        chosen = jnp.logical_or(chosen, ids[:, k:k + 1] == lane_e)
    top = jnp.max(jnp.where(chosen, logits, -jnp.inf), axis=-1, keepdims=True)
    weight = jnp.where(chosen, jnp.exp(jnp.where(chosen, logits - top, 0.0)), 0.0)
    gates = jnp.where(chosen, weight / jnp.sum(weight, axis=-1, keepdims=True), -1.0)
    gate[pl.ds(own * tok, tok), :] = jnp.concatenate([gates, jnp.full((tok, 128 - experts), -1.0, F32)], axis=1)
    send_g(own, TO_Z, TO_Y, TO_C, TO_F0, TO_F1)
    for s in range(2):
        send_h(own, s, TO_F0, TO_F1)

    bgu[...] = bgu_ref[...].astype(F32)
    bd[...] = bd_ref[...].astype(F32)
    pi, pj = iota((256, 256), 0), iota((256, 256), 1)
    perm[...] = (lax.div(pi, 2) + 128 * lax.rem(pi, 2) == pj).astype(F32).astype(BF16)

    for s in range(2):
        pass_h(near, s, TO_Y, TO_C)
        pass_h(y_own, s, TO_C)
    pass_g(near, TO_Y, TO_C)
    pass_g(y_own, TO_C)
    for s in range(2):
        pass_h(y_near, s, TO_C)
    pass_g(y_near, TO_C)

    def finish_gather(q):
        for yy in range(2):
            for zz in range(2):
                b = pos(q, 1 - c, yy, zz)
                for s in range(2):
                    pass_h(b, s)
                pass_g(b)

    def forward_far():
        for b in far:
            pass_g(b, TO_Y, TO_C)
            for s in range(2):
                pass_h(b, s, TO_Y, TO_C)

    def forward_far_y():
        for b in y_far:
            pass_g(b, TO_C)
            for s in range(2):
                pass_h(b, s, TO_C)

    def route(q):
        g = gate[pl.ds(q * tc, tc), :]
        hit = g >= 0.0
        ri, rj = iota((tc, tc), 0), iota((tc, tc), 1)
        before = jnp.logical_and(rj < ri, lax.div(rj, tok) == lax.div(ri, tok)).astype(F32).astype(BF16)
        rank = dot(before, hit.astype(F32).astype(BF16))
        base = (lax.div(iota((tc, 128), 0), tok) * cap).astype(F32)
        slot = jnp.where(hit, rank + base, -1.0)
        slot_t[...] = slot.T
        lane = iota((tc, 128), 1)
        s_lane = iota((tc, ns), 1).astype(F32)
        s_row = iota((ns, tc), 0).astype(F32)
        for e in range(local_exp):
            col = me * local_exp + e
            pick = lane == col
            p_e = jnp.sum(jnp.where(pick, jnp.maximum(g, 0.0), 0.0), axis=1, keepdims=True)
            s_e = jnp.sum(jnp.where(pick, slot, 0.0), axis=1, keepdims=True)
            back[:, e * ns:(e + 1) * ns] = (s_e == s_lane).astype(F32).astype(BF16)
            pgate[:, e * 128:(e + 1) * 128] = jnp.broadcast_to(p_e, (tc, 128))
            sel[e * ns:(e + 1) * ns, :] = (slot_t[pl.ds(col, 1), :] == s_row).astype(F32).astype(BF16)

    nb_w = 512
    def gate_up(e, q):
        pick = sel[pl.ds(e * ns, ns), :]
        valid = jnp.max(pick.astype(F32), axis=1, keepdims=True) > 0.0
        for i in range(d_model // nb_w):
            sl = slice(i * nb_w, (i + 1) * nb_w)
            rows[:, sl] = dot(pick, hid[pl.ds(q * tc, tc), sl]).astype(BF16)
        for i in range(2 * d_ff // nb_w):
            sl = slice(i * nb_w, (i + 1) * nb_w)
            u = (dot(rows[...], wgu[e, :, sl]) + bgu[pl.ds(e, 1), sl]).astype(BF16)
            for j in range(nb_w // 256):
                v = dot(u[:, j * 256:(j + 1) * 256], perm[...])
                a = jnp.minimum(v[:, :128], LIMIT)
                l = jnp.clip(v[:, 128:], -LIMIT, LIMIT)
                o = a * jax.nn.sigmoid(ALPHA * a) * (l + 1.0)
                m = i * (nb_w // 256) + j
                glu[e, :, m * 128:(m + 1) * 128] = jnp.where(valid, o, 0.0).astype(BF16)

    per = PIECES // STEPS

    def down(n, k):
        cols = pl.ds(pl.multiple_of(n * (per * cw), 128), per * cw)
        for e in range(local_exp):
            y_e = (dot(glu[e], wd[e, :, cols]) + bd[e:e + 1, cols]).astype(BF16)
            t = dot(back[:, e * ns:(e + 1) * ns], y_e)
            p_e = pgate[:, e * 128:(e + 1) * 128]
            for i in range(per):
                for j in range(cw // 128):
                    js = slice(j * 128, (j + 1) * 128)
                    ts = slice(i * cw + j * 128, i * cw + (j + 1) * 128)
                    if e == 0:
                        acc[k, n * per + i, :, js] = p_e * t[:, ts]
                    else:
                        acc[k, n * per + i, :, js] += p_e * t[:, ts]

    mine = (c * 2 + y) * 2 * tok

    def core_copy(k, n):
        return remote(acc.at[k, n, pl.ds((1 - c) * 4 * tok, 4 * tok)], r_core.at[k, n], s_core.at[k, n], q_core.at[k, n], partner)

    def y_copy(k, n):
        return remote(acc.at[k, n, pl.ds((c * 2 + 1 - y) * 2 * tok, 2 * tok)], r_y.at[k, n], s_y.at[k, n], q_y.at[k, n], ypeer)

    def near_copy(n):
        return remote(acc.at[0, n, pl.ds(mine + (1 - zin) * tok, tok)], r_z.at[2, n], s_z.at[2, n], q_z.at[2, n], zpeer)

    def far_copy(j, n):
        return remote(acc.at[1, n, pl.ds(mine + j * tok, tok)], r_z.at[zin, n], s_z.at[j, n], q_z.at[zin, n], zfar[j])

    def far_wait(j, n):
        remote(acc.at[1, n, pl.ds(mine + j * tok, tok)], r_z.at[j, n], s_z.at[j, n], q_z.at[j, n], zfar[j]).wait_recv()

    def start_core(k, n):
        for i in range(per):
            core_copy(k, n * per + i).start()

    def after_core(k, m):
        for i in range(per):
            n = m * per + i
            core_copy(k, n).wait_recv()
            acc[k, n, pl.ds((c * 2 + 1 - y) * 2 * tok, 2 * tok)] += r_core[k, n, pl.ds((1 - y) * 2 * tok, 2 * tok)]
            y_copy(k, n).start()
            acc[k, n, pl.ds(mine, 2 * tok)] += r_core[k, n, pl.ds(y * 2 * tok, 2 * tok)]

    def after_y(k, n):
        y_copy(k, n).wait_recv()
        acc[k, n, pl.ds(mine, 2 * tok)] += r_y[k, n]
        if k == 0:
            near_copy(n).start()
        else:
            for j in range(2):
                far_copy(j, n).start()

    def finish(n):
        near_copy(n).wait_recv()
        for j in range(2):
            far_wait(j, n)
        cols = slice(n * cw, (n + 1) * cw)
        total = acc[0, n, pl.ds(mine + zin * tok, tok)] + r_z[2, n]
        total = total + (r_z[0, n] + r_z[1, n])
        out_ref[:, cols] = (x_ref[:, cols].astype(F32) + total).astype(BF16)

    finish_gather(pair)
    route(pair)

    def up0(e, _):
        for i in range(local_exp):
            @pl.when(e == i)
            def _():
                w_copy(i).wait()
        gate_up(e, pair)

        @pl.when(e == 1)
        def _():
            forward_far()

        @pl.when(e == 3)
        def _():
            forward_far_y()
        return 0
    lax.fori_loop(0, local_exp, up0, 0)
    for i in range(local_exp, 2 * local_exp):
        w_copy(i).wait()

    def down0(n, _):
        down(n, 0)
        start_core(0, n)

        @pl.when(n > 0)
        def _():
            after_core(0, n - 1)
        return 0
    lax.fori_loop(0, STEPS, down0, 0)

    finish_gather(1 - pair)
    after_core(0, STEPS - 1)
    route(1 - pair)

    def up1(e, _):
        gate_up(e, 1 - pair)
        for i in range(per):
            after_y(0, e * per + i)
        return 0
    lax.fori_loop(0, local_exp, up1, 0)

    def down1(n, _):
        down(n, 1)
        start_core(1, n)

        @pl.when(n > 0)
        def _():
            after_core(1, n - 1)
        return 0
    lax.fori_loop(0, STEPS, down1, 0)
    after_core(1, STEPS - 1)
    for n in range(PIECES):
        after_y(1, n)
    for n in range(PIECES):
        finish(n)

    sent(own, TO_Z, TO_Y, TO_C, TO_F0, TO_F1)
    for b in (near, *far):
        sent(b, TO_Y, TO_C)
    for b in (y_own, y_near, *y_far):
        sent(b, TO_C)
    for n in range(PIECES):
        for k in range(2):
            core_copy(k, n).wait_send()
            y_copy(k, n).wait_send()
            far_copy(k, n).wait_send()
        near_copy(n).wait_send()


def solution(mesh):
    n_group = mesh.shape['ep']
    rows_spec = P(('dp', 'ep'), None)

    def local_block(x_in, expert_ids, norm_weight, router_w, router_b, w_gate_up, b_gate_up, w_down, b_down):
        tok, d_model = x_in.shape
        top_k = expert_ids.shape[1]
        local_exp, d_ff = w_down.shape[0], w_down.shape[1]
        experts = local_exp * n_group
        cap = CAPACITY_FACTOR * top_k * tok // experts
        cfg = (tok, d_model, d_ff, top_k, experts, local_exp, cap)
        tc, ns, cw = 8 * tok, 8 * cap, d_model // PIECES
        vm = pl.BlockSpec(memory_space=pltpu.VMEM)
        hbm = pl.BlockSpec(memory_space=pl.ANY)
        dma = pltpu.SemaphoreType.DMA
        return pl.pallas_call(
            functools.partial(moe_kernel, cfg),
            out_shape=jax.ShapeDtypeStruct((tok, d_model), BF16),
            in_specs=[vm, vm, vm, vm, vm, hbm, vm, hbm, vm],
            out_specs=vm,
            scratch_shapes=[
                pltpu.VMEM((local_exp, d_model, 2 * d_ff), BF16),
                pltpu.VMEM((local_exp, d_ff, d_model), BF16),
                pltpu.VMEM((n_group * tok, d_model), BF16),
                pltpu.VMEM((n_group * tok, 128), F32),
                pltpu.VMEM((local_exp * ns, tc), BF16),
                pltpu.VMEM((tc, local_exp * ns), BF16),
                pltpu.VMEM((tc, local_exp * 128), F32),
                pltpu.VMEM((128, tc), F32),
                pltpu.VMEM((ns, d_model), BF16),
                pltpu.VMEM((local_exp, ns, d_ff), BF16),
                pltpu.VMEM((256, 256), BF16),
                pltpu.VMEM((local_exp, 2 * d_ff), F32),
                pltpu.VMEM((local_exp, d_model), F32),
                pltpu.VMEM((2, PIECES, tc, cw), F32),
                pltpu.VMEM((2, PIECES, 4 * tok, cw), F32),
                pltpu.VMEM((2, PIECES, 2 * tok, cw), F32),
                pltpu.VMEM((3, PIECES, tok, cw), F32),
                dma((2 * local_exp,)),
                dma((5, n_group, 2)), dma((n_group, 2)), dma((5, n_group)), dma((n_group,)),
                dma((2, PIECES)), dma((2, PIECES)), dma((2, PIECES)), dma((2, PIECES)),
                dma((3, PIECES)), dma((3, PIECES)),
            ],
            compiler_params=pltpu.CompilerParams(
                collective_id=0, has_side_effects=True, vmem_limit_bytes=67043328),
            name='moe_block',
        )(x_in, expert_ids.T, norm_weight, router_w.T, router_b.reshape(1, -1), w_gate_up, b_gate_up, w_down, b_down)

    return jax.shard_map(local_block, mesh=mesh, in_specs=(rows_spec, rows_spec, P(), P(), P(), P('ep', None, None), P('ep', None), P('ep', None, None), P('ep', None)), out_specs=rows_spec, check_vma=False)
```

```python
import functools

import jax
import jax.numpy as jnp
from jax import lax
from jax.experimental import pallas as pl
from jax.experimental.pallas import tpu as pltpu
from jax.sharding import PartitionSpec as P

CAPACITY_FACTOR = 4
EPSILON = 1e-5
LIMIT = 7.0
ALPHA = 1.702
MESH = pl.DeviceIdType.MESH
PIECES = 8
STEPS = 4
F32 = jnp.float32
BF16 = jnp.bfloat16


def dot(a, b):
    return jnp.dot(a, b, preferred_element_type=F32)


def iota(shape, dim):
    return lax.broadcasted_iota(jnp.int32, shape, dim)


def moe_kernel(cfg, x_ref, ids_ref, g_ref, wr_ref, br_ref, wgu_hbm, bgu_ref, wd_hbm, bd_ref, out_ref,
               wgu, wd, hid, gate, sel, back, pgate, slot_t, rows, glu, perm, bgu, bd,
               acc, r_core, r_y, r_z,
               s_w, s_h, q_h, s_g, q_g, s_core, q_core, s_y, q_y, s_z, q_z):
    tok, d_model, d_ff, top_k, experts, local_exp, cap = cfg
    tc = 8 * tok
    ns = 8 * cap
    cw = d_model // PIECES
    half = tok // 2
    me = lax.axis_index('ep')
    z, y, c = lax.div(me, 4), lax.rem(lax.div(me, 2), 2), lax.rem(me, 2)
    pair, zin = lax.rem(z, 2), lax.div(z, 2)
    partner, ypeer, zpeer = me + 1 - 2 * c, me + 2 - 4 * y, me + 8 - 16 * zin
    zfar = [me + 4 * (2 * j + 1 - pair - z) for j in range(2)]

    def pos(q, cc, yy, zz):
        return ((q * 2 + cc) * 2 + yy) * 2 + zz

    def remote(src, dst, send, recv, dev):
        return pltpu.make_async_remote_copy(src_ref=src, dst_ref=dst, send_sem=send, recv_sem=recv,
                                            device_id={'ep': dev}, device_id_type=MESH)

    def w_copy(i):
        if i < local_exp:
            return pltpu.make_async_copy(wgu_hbm.at[i], wgu.at[i], s_w.at[i])
        return pltpu.make_async_copy(wd_hbm.at[i - local_exp], wd.at[i - local_exp], s_w.at[i])

    for i in range(2 * local_exp):
        w_copy(i).start()

    barrier = pltpu.get_barrier_semaphore()
    for dev in (partner, ypeer, zpeer, *zfar):
        pl.semaphore_signal(barrier, inc=1, device_id={'ep': dev}, device_id_type=MESH)

    own = pos(pair, c, y, zin)
    x = x_ref[...].astype(F32)
    inv = lax.rsqrt(jnp.mean(x * x, axis=-1, keepdims=True) + EPSILON)
    h = (x * inv * g_ref[...].reshape(1, d_model).astype(F32)).astype(BF16)
    hid[pl.ds(own * tok, tok), :] = h
    pl.semaphore_wait(barrier, 5)

    TO_Z, TO_Y, TO_C, TO_F0, TO_F1 = range(5)
    dest = [zpeer, ypeer, partner, zfar[0], zfar[1]]

    def h_copy(b, d, s):
        rs = pl.ds(b * tok + s * half, half)
        return remote(hid.at[rs], hid.at[rs], s_h.at[d, b, s], q_h.at[b, s], dest[d])

    def g_copy(b, d):
        rs = pl.ds(b * tok, tok)
        return remote(gate.at[rs], gate.at[rs], s_g.at[d, b], q_g.at[b], dest[d])

    def send_h(b, s, *ds):
        for d in ds:
            h_copy(b, d, s).start()

    def send_g(b, *ds):
        for d in ds:
            g_copy(b, d).start()

    def pass_h(b, s, *ds):
        h_copy(b, 0, s).wait_recv()
        send_h(b, s, *ds)

    def pass_g(b, *ds):
        g_copy(b, 0).wait_recv()
        send_g(b, *ds)

    def sent(b, *ds):
        for d in ds:
            for s in range(2):
                h_copy(b, d, s).wait_send()
            g_copy(b, d).wait_send()

    near = pos(pair, c, y, 1 - zin)
    y_own, y_near = pos(pair, c, 1 - y, zin), pos(pair, c, 1 - y, 1 - zin)
    first = lax.div(z, 3)
    far = [pos(1 - pair, c, y, j) for j in (first, 1 - first)]
    y_far = [pos(1 - pair, c, 1 - y, j) for j in (first, 1 - first)]

    for s in range(2):
        send_h(own, s, TO_Z, TO_Y)
    for s in range(2):
        send_h(own, s, TO_C)

    logits = lax.dot_general(h, wr_ref[...], (((1,), (1,)), ((), ())), preferred_element_type=F32) + br_ref[...].astype(F32)
    lane_e = iota((tok, experts), 1)
    ids = ids_ref[...].T
    chosen = ids[:, 0:1] == lane_e
    for k in range(1, top_k):
        chosen = jnp.logical_or(chosen, ids[:, k:k + 1] == lane_e)
    top = jnp.max(jnp.where(chosen, logits, -jnp.inf), axis=-1, keepdims=True)
    weight = jnp.where(chosen, jnp.exp(jnp.where(chosen, logits - top, 0.0)), 0.0)
    gates = jnp.where(chosen, weight / jnp.sum(weight, axis=-1, keepdims=True), -1.0)
    gate[pl.ds(own * tok, tok), :] = jnp.concatenate([gates, jnp.full((tok, 128 - experts), -1.0, F32)], axis=1)
    send_g(own, TO_Z, TO_Y, TO_C, TO_F0, TO_F1)
    for s in range(2):
        send_h(own, s, TO_F0, TO_F1)

    bgu[...] = bgu_ref[...].astype(F32)
    bd[...] = bd_ref[...].astype(F32)
    pi, pj = iota((256, 256), 0), iota((256, 256), 1)
    perm[...] = (lax.div(pi, 2) + 128 * lax.rem(pi, 2) == pj).astype(F32).astype(BF16)

    for s in range(2):
        pass_h(near, s, TO_Y, TO_C)
        pass_h(y_own, s, TO_C)
    pass_g(near, TO_Y, TO_C)
    pass_g(y_own, TO_C)
    for s in range(2):
        pass_h(y_near, s, TO_C)
    pass_g(y_near, TO_C)

    def finish_gather(q):
        for yy in range(2):
            for zz in range(2):
                b = pos(q, 1 - c, yy, zz)
                for s in range(2):
                    pass_h(b, s)
                pass_g(b)

    def forward_far(j):
        pass_g(far[j], TO_Y, TO_C)
        for s in range(2):
            pass_h(far[j], s, TO_Y, TO_C)

    def forward_far_y(j):
        pass_g(y_far[j], TO_C)
        for s in range(2):
            pass_h(y_far[j], s, TO_C)

    def route(q):
        g = gate[pl.ds(q * tc, tc), :]
        hit = g >= 0.0
        ri, rj = iota((tc, tc), 0), iota((tc, tc), 1)
        before = jnp.logical_and(rj < ri, lax.div(rj, tok) == lax.div(ri, tok)).astype(F32).astype(BF16)
        rank = dot(before, hit.astype(F32).astype(BF16))
        base = (lax.div(iota((tc, 128), 0), tok) * cap).astype(F32)
        slot = jnp.where(hit, rank + base, -1.0)
        slot_t[...] = slot.T
        lane = iota((tc, 128), 1)
        s_lane = iota((tc, ns), 1).astype(F32)
        s_row = iota((ns, tc), 0).astype(F32)
        for e in range(local_exp):
            col = me * local_exp + e
            pick = lane == col
            p_e = jnp.sum(jnp.where(pick, jnp.maximum(g, 0.0), 0.0), axis=1, keepdims=True)
            s_e = jnp.sum(jnp.where(pick, slot, 0.0), axis=1, keepdims=True)
            back[:, e * ns:(e + 1) * ns] = (s_e == s_lane).astype(F32).astype(BF16)
            pgate[:, e * 128:(e + 1) * 128] = jnp.broadcast_to(p_e, (tc, 128))
            sel[e * ns:(e + 1) * ns, :] = (slot_t[pl.ds(col, 1), :] == s_row).astype(F32).astype(BF16)

    def gate_up(e, q):
        pick = sel[e * ns:(e + 1) * ns, :]
        valid = jnp.max(pick.astype(F32), axis=1, keepdims=True) > 0.0
        rows[...] = dot(pick, hid[pl.ds(q * tc, tc), :]).astype(BF16)
        u = (dot(rows[...], wgu[e]) + bgu[e:e + 1, :]).astype(BF16)
        for j in range(2 * d_ff // 256):
            v = dot(u[:, j * 256:(j + 1) * 256], perm[...])
            a = jnp.minimum(v[:, :128], LIMIT)
            l = jnp.clip(v[:, 128:], -LIMIT, LIMIT)
            o = a * jax.nn.sigmoid(ALPHA * a) * (l + 1.0)
            glu[e, :, j * 128:(j + 1) * 128] = jnp.where(valid, o, 0.0).astype(BF16)

    per = PIECES // STEPS

    def down(n, k):
        cols = pl.ds(pl.multiple_of(n * (per * cw), 128), per * cw)
        ys = [(dot(glu[e], wd[e, :, cols]) + bd[e:e + 1, cols]).astype(BF16) for e in range(local_exp)]
        ts = [dot(back[:, e * ns:(e + 1) * ns], ys[e]) for e in range(local_exp)]
        for i in range(per):
            for j in range(cw // 128):
                sl = slice(i * cw + j * 128, i * cw + (j + 1) * 128)
                part = pgate[:, 0:128] * ts[0][:, sl]
                for e in range(1, local_exp):
                    part = part + pgate[:, e * 128:(e + 1) * 128] * ts[e][:, sl]
                acc[k, n * per + i, :, j * 128:(j + 1) * 128] = part

    mine = (c * 2 + y) * 2 * tok

    def core_copy(k, n):
        return remote(acc.at[k, n, pl.ds((1 - c) * 4 * tok, 4 * tok)], r_core.at[k, n], s_core.at[k, n], q_core.at[k, n], partner)

    def y_copy(k, n):
        return remote(acc.at[k, n, pl.ds((c * 2 + 1 - y) * 2 * tok, 2 * tok)], r_y.at[k, n], s_y.at[k, n], q_y.at[k, n], ypeer)

    def near_copy(n):
        return remote(acc.at[0, n, pl.ds(mine + (1 - zin) * tok, tok)], r_z.at[2, n], s_z.at[2, n], q_z.at[2, n], zpeer)

    def far_copy(j, n):
        return remote(acc.at[1, n, pl.ds(mine + j * tok, tok)], r_z.at[zin, n], s_z.at[j, n], q_z.at[zin, n], zfar[j])

    def far_wait(j, n):
        remote(acc.at[1, n, pl.ds(mine + j * tok, tok)], r_z.at[j, n], s_z.at[j, n], q_z.at[j, n], zfar[j]).wait_recv()

    def start_core(k, n):
        for i in range(per):
            core_copy(k, n * per + i).start()

    def after_core(k, m):
        for i in range(per):
            n = m * per + i
            core_copy(k, n).wait_recv()
            acc[k, n, pl.ds((c * 2 + 1 - y) * 2 * tok, 2 * tok)] += r_core[k, n, pl.ds((1 - y) * 2 * tok, 2 * tok)]
            y_copy(k, n).start()
            acc[k, n, pl.ds(mine, 2 * tok)] += r_core[k, n, pl.ds(y * 2 * tok, 2 * tok)]

    def after_y(k, n):
        y_copy(k, n).wait_recv()
        acc[k, n, pl.ds(mine, 2 * tok)] += r_y[k, n]
        if k == 0:
            near_copy(n).start()
        else:
            for j in range(2):
                far_copy(j, n).start()

    def finish(n):
        near_copy(n).wait_recv()
        for j in range(2):
            far_wait(j, n)
        cols = slice(n * cw, (n + 1) * cw)
        total = acc[0, n, pl.ds(mine + zin * tok, tok)] + r_z[2, n]
        total = total + (r_z[0, n] + r_z[1, n])
        out_ref[:, cols] = (x_ref[:, cols].astype(F32) + total).astype(BF16)

    finish_gather(pair)
    route(pair)

    for e in range(local_exp):
        w_copy(e).wait()
        gate_up(e, pair)
        if e < 2:
            forward_far(e)
    for i in range(local_exp, 2 * local_exp):
        w_copy(i).wait()

    def down0(n, _):
        down(n, 0)
        start_core(0, n)

        @pl.when(n > 0)
        def _():
            after_core(0, n - 1)

        @pl.when(n == 1)
        def _():
            forward_far_y(0)

        @pl.when(n == 3)
        def _():
            forward_far_y(1)
        return 0
    lax.fori_loop(0, STEPS, down0, 0)

    after_core(0, STEPS - 1)
    finish_gather(1 - pair)
    route(1 - pair)
    for e in range(local_exp):
        gate_up(e, 1 - pair)
        for i in range(per):
            after_y(0, e * per + i)

    def down1(n, _):
        down(n, 1)
        start_core(1, n)

        @pl.when(n > 0)
        def _():
            after_core(1, n - 1)
        return 0
    lax.fori_loop(0, STEPS, down1, 0)
    after_core(1, STEPS - 1)
    for n in range(PIECES):
        after_y(1, n)
    for n in range(PIECES):
        finish(n)

    sent(own, TO_Z, TO_Y, TO_C, TO_F0, TO_F1)
    for b in (near, *far):
        sent(b, TO_Y, TO_C)
    for b in (y_own, y_near, *y_far):
        sent(b, TO_C)
    for n in range(PIECES):
        for k in range(2):
            core_copy(k, n).wait_send()
            y_copy(k, n).wait_send()
            far_copy(k, n).wait_send()
        near_copy(n).wait_send()


def solution(mesh):
    n_group = mesh.shape['ep']
    rows_spec = P(('dp', 'ep'), None)

    def local_block(x_in, expert_ids, norm_weight, router_w, router_b, w_gate_up, b_gate_up, w_down, b_down):
        tok, d_model = x_in.shape
        top_k = expert_ids.shape[1]
        local_exp, d_ff = w_down.shape[0], w_down.shape[1]
        experts = local_exp * n_group
        cap = CAPACITY_FACTOR * top_k * tok // experts
        cfg = (tok, d_model, d_ff, top_k, experts, local_exp, cap)
        tc, ns, cw = 8 * tok, 8 * cap, d_model // PIECES
        vm = pl.BlockSpec(memory_space=pltpu.VMEM)
        hbm = pl.BlockSpec(memory_space=pl.ANY)
        dma = pltpu.SemaphoreType.DMA
        return pl.pallas_call(
            functools.partial(moe_kernel, cfg),
            out_shape=jax.ShapeDtypeStruct((tok, d_model), BF16),
            in_specs=[vm, vm, vm, vm, vm, hbm, vm, hbm, vm],
            out_specs=vm,
            scratch_shapes=[
                pltpu.VMEM((local_exp, d_model, 2 * d_ff), BF16),
                pltpu.VMEM((local_exp, d_ff, d_model), BF16),
                pltpu.VMEM((n_group * tok, d_model), BF16),
                pltpu.VMEM((n_group * tok, 128), F32),
                pltpu.VMEM((local_exp * ns, tc), BF16),
                pltpu.VMEM((tc, local_exp * ns), BF16),
                pltpu.VMEM((tc, local_exp * 128), F32),
                pltpu.VMEM((128, tc), F32),
                pltpu.VMEM((ns, d_model), BF16),
                pltpu.VMEM((local_exp, ns, d_ff), BF16),
                pltpu.VMEM((256, 256), BF16),
                pltpu.VMEM((local_exp, 2 * d_ff), F32),
                pltpu.VMEM((local_exp, d_model), F32),
                pltpu.VMEM((2, PIECES, tc, cw), F32),
                pltpu.VMEM((2, PIECES, 4 * tok, cw), F32),
                pltpu.VMEM((2, PIECES, 2 * tok, cw), F32),
                pltpu.VMEM((3, PIECES, tok, cw), F32),
                dma((2 * local_exp,)),
                dma((5, n_group, 2)), dma((n_group, 2)), dma((5, n_group)), dma((n_group,)),
                dma((2, PIECES)), dma((2, PIECES)), dma((2, PIECES)), dma((2, PIECES)),
                dma((3, PIECES)), dma((3, PIECES)),
            ],
            compiler_params=pltpu.CompilerParams(
                collective_id=0, has_side_effects=True, vmem_limit_bytes=67043328),
            name='moe_block',
        )(x_in, expert_ids.T, norm_weight, router_w.T, router_b.reshape(1, -1), w_gate_up, b_gate_up, w_down, b_down)

    return jax.shard_map(local_block, mesh=mesh, in_specs=(rows_spec, rows_spec, P(), P(), P(), P('ep', None, None), P('ep', None), P('ep', None, None), P('ep', None)), out_specs=rows_spec, check_vma=False)
```

```python
import functools

import jax
import jax.numpy as jnp
from jax import lax
from jax.experimental import pallas as pl
from jax.experimental.pallas import tpu as pltpu
from jax.sharding import PartitionSpec as P

CAPACITY_FACTOR = 4
EPSILON = 1e-5
LIMIT = 7.0
ALPHA = 1.702
MESH = pl.DeviceIdType.MESH
PIECES = 4
STEPS = 4
F32 = jnp.float32
BF16 = jnp.bfloat16


def dot(a, b):
    return jnp.dot(a, b, preferred_element_type=F32)


def iota(shape, dim):
    return lax.broadcasted_iota(jnp.int32, shape, dim)


def moe_kernel(cfg, x_ref, ids_ref, g_ref, wr_ref, br_ref, wgu_hbm, bgu_ref, wd_hbm, bd_ref, out_ref,
               wgu, wd, hid, gate, sel, back, pgate, slot_t, rows, glu, perm, bgu, bd,
               acc, r_core, r_y, r_z,
               s_w, s_h, q_h, s_g, q_g, s_core, q_core, s_y, q_y, s_z, q_z):
    tok, d_model, d_ff, top_k, experts, local_exp, cap = cfg
    tc = 8 * tok
    ns = 8 * cap
    cw = d_model // PIECES
    half = tok // 2
    me = lax.axis_index('ep')
    z, y, c = lax.div(me, 4), lax.rem(lax.div(me, 2), 2), lax.rem(me, 2)
    pair, zin = lax.rem(z, 2), lax.div(z, 2)
    partner, ypeer, zpeer = me + 1 - 2 * c, me + 2 - 4 * y, me + 8 - 16 * zin
    zfar = [me + 4 * (2 * j + 1 - pair - z) for j in range(2)]
    is_mid = zin != pair

    def pos(q, cc, yy, zz):
        return ((q * 2 + cc) * 2 + yy) * 2 + zz

    def remote(src, dst, send, recv, dev):
        return pltpu.make_async_remote_copy(src_ref=src, dst_ref=dst, send_sem=send, recv_sem=recv,
                                            device_id={'ep': dev}, device_id_type=MESH)

    def w_copy(i):
        if i < local_exp:
            return pltpu.make_async_copy(wgu_hbm.at[i], wgu.at[i], s_w.at[i])
        return pltpu.make_async_copy(wd_hbm.at[i - local_exp], wd.at[i - local_exp], s_w.at[i])

    for i in range(2 * local_exp):
        w_copy(i).start()

    barrier = pltpu.get_barrier_semaphore()
    for dev in (partner, ypeer, zpeer, *zfar):
        pl.semaphore_signal(barrier, inc=1, device_id={'ep': dev}, device_id_type=MESH)

    own = pos(pair, c, y, zin)
    x = x_ref[...].astype(F32)
    inv = lax.rsqrt(jnp.mean(x * x, axis=-1, keepdims=True) + EPSILON)
    h = (x * inv * g_ref[...].reshape(1, d_model).astype(F32)).astype(BF16)
    hid[pl.ds(own * tok, tok), :] = h
    pl.semaphore_wait(barrier, 5)

    TO_Z, TO_Y, TO_C, TO_F0, TO_F1 = range(5)
    dest = [zpeer, ypeer, partner, me + 4 * (2 * zin + 1 - pair - z), me + 4 * (3 - 2 * zin - pair - z)]

    def h_copy(b, d, s):
        rs = pl.ds(b * tok + s * half, half)
        return remote(hid.at[rs], hid.at[rs], s_h.at[d, b, s], q_h.at[b, s], dest[d])

    def g_copy(b, d):
        rs = pl.ds(b * tok, tok)
        return remote(gate.at[rs], gate.at[rs], s_g.at[d, b], q_g.at[b], dest[d])

    def send_h(b, s, *ds):
        for d in ds:
            h_copy(b, d, s).start()

    def send_g(b, *ds):
        for d in ds:
            g_copy(b, d).start()

    def pass_h(b, s, *ds):
        h_copy(b, 0, s).wait_recv()
        send_h(b, s, *ds)

    def pass_g(b, *ds):
        g_copy(b, 0).wait_recv()
        send_g(b, *ds)

    def sent(b, *ds):
        for d in ds:
            for s in range(2):
                h_copy(b, d, s).wait_send()
            g_copy(b, d).wait_send()

    near = pos(pair, c, y, 1 - zin)
    y_own, y_near = pos(pair, c, 1 - y, zin), pos(pair, c, 1 - y, 1 - zin)
    far = [pos(1 - pair, c, y, j) for j in (zin, 1 - zin)]
    y_far = [pos(1 - pair, c, 1 - y, j) for j in (zin, 1 - zin)]

    for s in range(2):
        send_h(own, s, TO_Z, TO_Y)
    for s in range(2):
        send_h(own, s, TO_C)

    logits = lax.dot_general(h, wr_ref[...], (((1,), (1,)), ((), ())), preferred_element_type=F32) + br_ref[...].astype(F32)
    lane_e = iota((tok, experts), 1)
    ids = ids_ref[...].T
    chosen = ids[:, 0:1] == lane_e
    for k in range(1, top_k):
        chosen = jnp.logical_or(chosen, ids[:, k:k + 1] == lane_e)
    top = jnp.max(jnp.where(chosen, logits, -jnp.inf), axis=-1, keepdims=True)
    weight = jnp.where(chosen, jnp.exp(jnp.where(chosen, logits - top, 0.0)), 0.0)
    gates = jnp.where(chosen, weight / jnp.sum(weight, axis=-1, keepdims=True), -1.0)
    gate[pl.ds(own * tok, tok), :] = jnp.concatenate([gates, jnp.full((tok, 128 - experts), -1.0, F32)], axis=1)
    send_g(own, TO_Z, TO_Y, TO_C, TO_F0)
    for s in range(2):
        send_h(own, s, TO_F0)

    @pl.when(is_mid)
    def _():
        send_g(own, TO_F1)
        for s in range(2):
            send_h(own, s, TO_F1)

    bgu[...] = bgu_ref[...].astype(F32)
    bd[...] = bd_ref[...].astype(F32)
    pi, pj = iota((256, 256), 0), iota((256, 256), 1)
    perm[...] = (lax.div(pi, 2) + 128 * lax.rem(pi, 2) == pj).astype(F32).astype(BF16)

    for s in range(2):
        pass_h(near, s, TO_Y, TO_C)
        pass_h(y_own, s, TO_C)
    pass_g(near, TO_Y, TO_C)
    pass_g(y_own, TO_C)

    @pl.when(is_mid)
    def _():
        send_g(near, TO_F0)
        for s in range(2):
            send_h(near, s, TO_F0)
    for s in range(2):
        pass_h(y_near, s, TO_C)
    pass_g(y_near, TO_C)

    def finish_gather(q):
        for yy in range(2):
            for zz in range(2):
                b = pos(q, 1 - c, yy, zz)
                for s in range(2):
                    pass_h(b, s)
                pass_g(b)

    def forward_far(j):
        pass_g(far[j], TO_Y, TO_C)
        for s in range(2):
            pass_h(far[j], s, TO_Y, TO_C)

    def forward_far_y(j):
        pass_g(y_far[j], TO_C)
        for s in range(2):
            pass_h(y_far[j], s, TO_C)

    def route(q):
        g = gate[pl.ds(q * tc, tc), :]
        hit = g >= 0.0
        ri, rj = iota((tc, tc), 0), iota((tc, tc), 1)
        before = jnp.logical_and(rj < ri, lax.div(rj, tok) == lax.div(ri, tok)).astype(F32).astype(BF16)
        rank = dot(before, hit.astype(F32).astype(BF16))
        base = (lax.div(iota((tc, 128), 0), tok) * cap).astype(F32)
        slot = jnp.where(hit, rank + base, -1.0)
        slot_t[...] = slot.T
        lane = iota((tc, 128), 1)
        s_lane = iota((tc, ns), 1).astype(F32)
        s_row = iota((ns, tc), 0).astype(F32)
        for e in range(local_exp):
            col = me * local_exp + e
            pick = lane == col
            p_e = jnp.sum(jnp.where(pick, jnp.maximum(g, 0.0), 0.0), axis=1, keepdims=True)
            s_e = jnp.sum(jnp.where(pick, slot, 0.0), axis=1, keepdims=True)
            back[:, e * ns:(e + 1) * ns] = (s_e == s_lane).astype(F32).astype(BF16)
            pgate[:, e * 128:(e + 1) * 128] = jnp.broadcast_to(p_e, (tc, 128))
            sel[e * ns:(e + 1) * ns, :] = (slot_t[pl.ds(col, 1), :] == s_row).astype(F32).astype(BF16)

    def gate_up(e, q):
        pick = sel[e * ns:(e + 1) * ns, :]
        valid = jnp.max(pick.astype(F32), axis=1, keepdims=True) > 0.0
        rows[...] = dot(pick, hid[pl.ds(q * tc, tc), :]).astype(BF16)
        u = (dot(rows[...], wgu[e]) + bgu[e:e + 1, :]).astype(BF16)
        for j in range(2 * d_ff // 256):
            v = dot(u[:, j * 256:(j + 1) * 256], perm[...])
            a = jnp.minimum(v[:, :128], LIMIT)
            l = jnp.clip(v[:, 128:], -LIMIT, LIMIT)
            o = a * jax.nn.sigmoid(ALPHA * a) * (l + 1.0)
            glu[e, :, j * 128:(j + 1) * 128] = jnp.where(valid, o, 0.0).astype(BF16)

    per = PIECES // STEPS

    def down(n, k):
        cols = pl.ds(pl.multiple_of(n * (per * cw), 128), per * cw)
        ys = [(dot(glu[e], wd[e, :, cols]) + bd[e:e + 1, cols]).astype(BF16) for e in range(local_exp)]
        ts = [dot(back[:, e * ns:(e + 1) * ns], ys[e]) for e in range(local_exp)]
        for i in range(per):
            for j in range(cw // 128):
                sl = slice(i * cw + j * 128, i * cw + (j + 1) * 128)
                part = pgate[:, 0:128] * ts[0][:, sl]
                for e in range(1, local_exp):
                    part = part + pgate[:, e * 128:(e + 1) * 128] * ts[e][:, sl]
                acc[k, n * per + i, :, j * 128:(j + 1) * 128] = part

    mine = (c * 2 + y) * 2 * tok

    def core_copy(k, n):
        return remote(acc.at[k, n, pl.ds((1 - c) * 4 * tok, 4 * tok)], r_core.at[k, n], s_core.at[k, n], q_core.at[k, n], partner)

    def y_copy(k, n):
        return remote(acc.at[k, n, pl.ds((c * 2 + 1 - y) * 2 * tok, 2 * tok)], r_y.at[k, n], s_y.at[k, n], q_y.at[k, n], ypeer)

    def near_copy(n):
        return remote(acc.at[0, n, pl.ds(mine + (1 - zin) * tok, tok)], r_z.at[2, n], s_z.at[2, n], q_z.at[2, n], zpeer)

    def far_copy(j, n):
        return remote(acc.at[1, n, pl.ds(mine + j * tok, tok)], r_z.at[zin, n], s_z.at[j, n], q_z.at[zin, n], zfar[j])

    def far_wait(j, n):
        remote(acc.at[1, n, pl.ds(mine + j * tok, tok)], r_z.at[j, n], s_z.at[j, n], q_z.at[j, n], zfar[j]).wait_recv()

    def start_core(k, n):
        for i in range(per):
            core_copy(k, n * per + i).start()

    def after_core(k, m):
        for i in range(per):
            n = m * per + i
            core_copy(k, n).wait_recv()
            acc[k, n, pl.ds((c * 2 + 1 - y) * 2 * tok, 2 * tok)] += r_core[k, n, pl.ds((1 - y) * 2 * tok, 2 * tok)]
            y_copy(k, n).start()
            acc[k, n, pl.ds(mine, 2 * tok)] += r_core[k, n, pl.ds(y * 2 * tok, 2 * tok)]

    def after_y(k, n):
        y_copy(k, n).wait_recv()
        acc[k, n, pl.ds(mine, 2 * tok)] += r_y[k, n]
        if k == 0:
            near_copy(n).start()
        else:
            for j in range(2):
                far_copy(j, n).start()

    def finish(n):
        near_copy(n).wait_recv()
        for j in range(2):
            far_wait(j, n)
        cols = slice(n * cw, (n + 1) * cw)
        total = acc[0, n, pl.ds(mine + zin * tok, tok)] + r_z[2, n]
        total = total + (r_z[0, n] + r_z[1, n])
        out_ref[:, cols] = (x_ref[:, cols].astype(F32) + total).astype(BF16)

    finish_gather(pair)
    forward_far(0)
    route(pair)

    for e in range(local_exp):
        w_copy(e).wait()
        gate_up(e, pair)
        if e == 1:
            forward_far(1)
        if e == 3:
            forward_far_y(0)
    for i in range(local_exp, 2 * local_exp):
        w_copy(i).wait()

    def down0(n, _):
        down(n, 0)
        start_core(0, n)

        @pl.when(n > 0)
        def _():
            after_core(0, n - 1)

        @pl.when(n == 2)
        def _():
            forward_far_y(1)
        return 0
    lax.fori_loop(0, STEPS, down0, 0)

    after_core(0, STEPS - 1)
    finish_gather(1 - pair)
    route(1 - pair)
    for e in range(local_exp):
        gate_up(e, 1 - pair)
        if e % 2 == 1:
            for i in range(per):
                after_y(0, (e // 2) * per + i)

    def down1(n, _):
        down(n, 1)
        start_core(1, n)

        @pl.when(n > 0)
        def _():
            after_core(1, n - 1)

        @pl.when(n == 2)
        def _():
            for i in range(per):
                after_y(0, 2 * per + i)
        return 0
    lax.fori_loop(0, STEPS, down1, 0)
    after_core(1, STEPS - 1)
    for i in range(per):
        after_y(0, 3 * per + i)
    for n in range(PIECES):
        after_y(1, n)
    for n in range(PIECES):
        finish(n)

    sent(own, TO_Z, TO_Y, TO_C, TO_F0)

    @pl.when(is_mid)
    def _():
        sent(own, TO_F1)
        sent(near, TO_F0)
    for b in (near, *far):
        sent(b, TO_Y, TO_C)
    for b in (y_own, y_near, *y_far):
        sent(b, TO_C)
    for n in range(PIECES):
        for k in range(2):
            core_copy(k, n).wait_send()
            y_copy(k, n).wait_send()
            far_copy(k, n).wait_send()
        near_copy(n).wait_send()


def solution(mesh):
    n_group = mesh.shape['ep']
    rows_spec = P(('dp', 'ep'), None)

    def local_block(x_in, expert_ids, norm_weight, router_w, router_b, w_gate_up, b_gate_up, w_down, b_down):
        tok, d_model = x_in.shape
        top_k = expert_ids.shape[1]
        local_exp, d_ff = w_down.shape[0], w_down.shape[1]
        experts = local_exp * n_group
        cap = CAPACITY_FACTOR * top_k * tok // experts
        cfg = (tok, d_model, d_ff, top_k, experts, local_exp, cap)
        tc, ns, cw = 8 * tok, 8 * cap, d_model // PIECES
        vm = pl.BlockSpec(memory_space=pltpu.VMEM)
        hbm = pl.BlockSpec(memory_space=pl.ANY)
        dma = pltpu.SemaphoreType.DMA
        return pl.pallas_call(
            functools.partial(moe_kernel, cfg),
            out_shape=jax.ShapeDtypeStruct((tok, d_model), BF16),
            in_specs=[vm, vm, vm, vm, vm, hbm, vm, hbm, vm],
            out_specs=vm,
            scratch_shapes=[
                pltpu.VMEM((local_exp, d_model, 2 * d_ff), BF16),
                pltpu.VMEM((local_exp, d_ff, d_model), BF16),
                pltpu.VMEM((n_group * tok, d_model), BF16),
                pltpu.VMEM((n_group * tok, 128), F32),
                pltpu.VMEM((local_exp * ns, tc), BF16),
                pltpu.VMEM((tc, local_exp * ns), BF16),
                pltpu.VMEM((tc, local_exp * 128), F32),
                pltpu.VMEM((128, tc), F32),
                pltpu.VMEM((ns, d_model), BF16),
                pltpu.VMEM((local_exp, ns, d_ff), BF16),
                pltpu.VMEM((256, 256), BF16),
                pltpu.VMEM((local_exp, 2 * d_ff), F32),
                pltpu.VMEM((local_exp, d_model), F32),
                pltpu.VMEM((2, PIECES, tc, cw), F32),
                pltpu.VMEM((2, PIECES, 4 * tok, cw), F32),
                pltpu.VMEM((2, PIECES, 2 * tok, cw), F32),
                pltpu.VMEM((3, PIECES, tok, cw), F32),
                dma((2 * local_exp,)),
                dma((5, n_group, 2)), dma((n_group, 2)), dma((5, n_group)), dma((n_group,)),
                dma((2, PIECES)), dma((2, PIECES)), dma((2, PIECES)), dma((2, PIECES)),
                dma((3, PIECES)), dma((3, PIECES)),
            ],
            compiler_params=pltpu.CompilerParams(
                collective_id=0, has_side_effects=True, vmem_limit_bytes=67043328),
            name='moe_block',
        )(x_in, expert_ids.T, norm_weight, router_w.T, router_b.reshape(1, -1), w_gate_up, b_gate_up, w_down, b_down)

    return jax.shard_map(local_block, mesh=mesh, in_specs=(rows_spec, rows_spec, P(), P(), P(), P('ep', None, None), P('ep', None), P('ep', None, None), P('ep', None)), out_specs=rows_spec, check_vma=False)
```

```python
import functools

import jax
import jax.numpy as jnp
from jax import lax
from jax.experimental import pallas as pl
from jax.experimental.pallas import tpu as pltpu
from jax.sharding import PartitionSpec as P

CAPACITY_FACTOR = 4
EPSILON = 1e-5
LIMIT = 7.0
ALPHA = 1.702
MESH = pl.DeviceIdType.MESH
PIECES = 4
STEPS = 4
F32 = jnp.float32
BF16 = jnp.bfloat16


def dot(a, b):
    return jnp.dot(a, b, preferred_element_type=F32)


def iota(shape, dim):
    return lax.broadcasted_iota(jnp.int32, shape, dim)


def moe_kernel(cfg, x_ref, ids_ref, g_ref, wr_ref, br_ref, wgu_hbm, bgu_ref, wd_hbm, bd_ref, out_ref,
               wgu, wd, hid, gate, sel, back, pgate, slot_t, rows, glu, perm, bgu, bd,
               acc, r_core, r_y, r_z,
               s_w, s_h, q_h, s_g, q_g, s_core, q_core, s_y, q_y, s_z, q_z):
    tok, d_model, d_ff, top_k, experts, local_exp, cap = cfg
    tc = 8 * tok
    ns = 8 * cap
    cw = d_model // PIECES
    half = tok // 2
    me = lax.axis_index('ep')
    z, y, c = lax.div(me, 4), lax.rem(lax.div(me, 2), 2), lax.rem(me, 2)
    pair, zin = lax.rem(z, 2), lax.div(z, 2)
    partner, ypeer, zpeer = me + 1 - 2 * c, me + 2 - 4 * y, me + 8 - 16 * zin
    zfar = [me + 4 * (2 * j + 1 - pair - z) for j in range(2)]
    is_mid = zin != pair

    def pos(q, cc, yy, zz):
        return ((q * 2 + cc) * 2 + yy) * 2 + zz

    def remote(src, dst, send, recv, dev):
        return pltpu.make_async_remote_copy(src_ref=src, dst_ref=dst, send_sem=send, recv_sem=recv,
                                            device_id={'ep': dev}, device_id_type=MESH)

    def w_copy(i):
        if i < local_exp:
            return pltpu.make_async_copy(wgu_hbm.at[i], wgu.at[i], s_w.at[i])
        return pltpu.make_async_copy(wd_hbm.at[i - local_exp], wd.at[i - local_exp], s_w.at[i])

    for i in range(2 * local_exp):
        w_copy(i).start()

    barrier = pltpu.get_barrier_semaphore()
    for dev in (partner, ypeer, zpeer, *zfar):
        pl.semaphore_signal(barrier, inc=1, device_id={'ep': dev}, device_id_type=MESH)

    own = pos(pair, c, y, zin)
    x = x_ref[...].astype(F32)
    inv = lax.rsqrt(jnp.mean(x * x, axis=-1, keepdims=True) + EPSILON)
    h = (x * inv * g_ref[...].reshape(1, d_model).astype(F32)).astype(BF16)
    hid[pl.ds(own * tok, tok), :] = h
    pl.semaphore_wait(barrier, 5)

    TO_Z, TO_Y, TO_C, TO_F0, TO_F1 = range(5)
    dest = [zpeer, ypeer, partner, me + 4 * (2 * zin + 1 - pair - z), me + 4 * (3 - 2 * zin - pair - z)]

    def h_copy(b, d, s):
        rs = pl.ds(b * tok + s * half, half)
        return remote(hid.at[rs], hid.at[rs], s_h.at[d, b, s], q_h.at[b, s], dest[d])

    def g_copy(b, d):
        rs = pl.ds(b * half, half)
        return remote(gate.at[rs], gate.at[rs], s_g.at[d, b], q_g.at[b], dest[d])

    def send_h(b, s, *ds):
        for d in ds:
            h_copy(b, d, s).start()

    def send_g(b, *ds):
        for d in ds:
            g_copy(b, d).start()

    def pass_h(b, s, *ds):
        h_copy(b, 0, s).wait_recv()
        send_h(b, s, *ds)

    def pass_g(b, *ds):
        g_copy(b, 0).wait_recv()
        send_g(b, *ds)

    def sent(b, *ds):
        for d in ds:
            for s in range(2):
                h_copy(b, d, s).wait_send()
            g_copy(b, d).wait_send()

    near = pos(pair, c, y, 1 - zin)
    y_own, y_near = pos(pair, c, 1 - y, zin), pos(pair, c, 1 - y, 1 - zin)
    far = [pos(1 - pair, c, y, j) for j in (zin, 1 - zin)]
    y_far = [pos(1 - pair, c, 1 - y, j) for j in (zin, 1 - zin)]

    for s in range(2):
        send_h(own, s, TO_Z, TO_Y)
    for s in range(2):
        send_h(own, s, TO_C)

    logits = lax.dot_general(h, wr_ref[...], (((1,), (1,)), ((), ())), preferred_element_type=F32) + br_ref[...].astype(F32)
    lane_e = iota((tok, experts), 1)
    ids = ids_ref[...].T
    chosen = ids[:, 0:1] == lane_e
    for k in range(1, top_k):
        chosen = jnp.logical_or(chosen, ids[:, k:k + 1] == lane_e)
    top = jnp.max(jnp.where(chosen, logits, -jnp.inf), axis=-1, keepdims=True)
    weight = jnp.where(chosen, jnp.exp(jnp.where(chosen, logits - top, 0.0)), 0.0)
    gates = jnp.where(chosen, weight / jnp.sum(weight, axis=-1, keepdims=True), -1.0)
    gate[pl.ds(own * half, half), :] = jnp.concatenate([gates[:half], gates[half:]], axis=1)
    send_g(own, TO_Z, TO_Y, TO_C, TO_F0)
    for s in range(2):
        send_h(own, s, TO_F0)

    @pl.when(is_mid)
    def _():
        send_g(own, TO_F1)
        for s in range(2):
            send_h(own, s, TO_F1)

    bgu[...] = bgu_ref[...].astype(F32)
    bd[...] = bd_ref[...].astype(F32)
    pi, pj = iota((256, 256), 0), iota((256, 256), 1)
    perm[...] = (lax.div(pi, 2) + 128 * lax.rem(pi, 2) == pj).astype(F32).astype(BF16)

    for s in range(2):
        pass_h(near, s, TO_Y, TO_C)
        pass_h(y_own, s, TO_C)
    pass_g(near, TO_Y, TO_C)
    pass_g(y_own, TO_C)

    @pl.when(is_mid)
    def _():
        send_g(near, TO_F0)
        for s in range(2):
            send_h(near, s, TO_F0)
    for s in range(2):
        pass_h(y_near, s, TO_C)
    pass_g(y_near, TO_C)

    def finish_gather(q):
        for yy in range(2):
            for zz in range(2):
                b = pos(q, 1 - c, yy, zz)
                for s in range(2):
                    pass_h(b, s)
                pass_g(b)

    def forward_far(j):
        pass_g(far[j], TO_Y, TO_C)
        for s in range(2):
            pass_h(far[j], s, TO_Y, TO_C)

    def forward_far_y(j):
        pass_g(y_far[j], TO_C)
        for s in range(2):
            pass_h(y_far[j], s, TO_C)

    def route(q):
        g2 = gate[pl.ds(q * 8 * half, 8 * half), :]
        g = jnp.concatenate([g2.reshape(8, half, 128), pltpu.roll(g2, experts, 1).reshape(8, half, 128)], axis=1).reshape(tc, 128)
        hit = g >= 0.0
        ri, rj = iota((tc, tc), 0), iota((tc, tc), 1)
        before = jnp.logical_and(rj < ri, lax.div(rj, tok) == lax.div(ri, tok)).astype(F32).astype(BF16)
        rank = dot(before, hit.astype(F32).astype(BF16))
        base = (lax.div(iota((tc, 128), 0), tok) * cap).astype(F32)
        slot = jnp.where(hit, rank + base, -1.0)
        slot_t[...] = slot.T
        lane = iota((tc, 128), 1)
        s_lane = iota((tc, ns), 1).astype(F32)
        s_row = iota((ns, tc), 0).astype(F32)
        for e in range(local_exp):
            col = me * local_exp + e
            pick = lane == col
            p_e = jnp.sum(jnp.where(pick, jnp.maximum(g, 0.0), 0.0), axis=1, keepdims=True)
            s_e = jnp.sum(jnp.where(pick, slot, 0.0), axis=1, keepdims=True)
            back[:, e * ns:(e + 1) * ns] = (s_e == s_lane).astype(F32).astype(BF16)
            pgate[:, e * 128:(e + 1) * 128] = jnp.broadcast_to(p_e, (tc, 128))
            sel[e * ns:(e + 1) * ns, :] = (slot_t[pl.ds(col, 1), :] == s_row).astype(F32).astype(BF16)

    def gate_up(e, q):
        pick = sel[e * ns:(e + 1) * ns, :]
        valid = jnp.max(pick.astype(F32), axis=1, keepdims=True) > 0.0
        rows[...] = dot(pick, hid[pl.ds(q * tc, tc), :]).astype(BF16)
        u = (dot(rows[...], wgu[e]) + bgu[e:e + 1, :]).astype(BF16)
        for j in range(2 * d_ff // 256):
            v = dot(u[:, j * 256:(j + 1) * 256], perm[...])
            a = jnp.minimum(v[:, :128], LIMIT)
            l = jnp.clip(v[:, 128:], -LIMIT, LIMIT)
            o = a * jax.nn.sigmoid(ALPHA * a) * (l + 1.0)
            glu[e, :, j * 128:(j + 1) * 128] = jnp.where(valid, o, 0.0).astype(BF16)

    per = PIECES // STEPS

    def down(n, k):
        cols = pl.ds(pl.multiple_of(n * (per * cw), 128), per * cw)
        ys = [(dot(glu[e], wd[e, :, cols]) + bd[e:e + 1, cols]).astype(BF16) for e in range(local_exp)]
        ts = [dot(back[:, e * ns:(e + 1) * ns], ys[e]) for e in range(local_exp)]
        for i in range(per):
            for j in range(cw // 128):
                sl = slice(i * cw + j * 128, i * cw + (j + 1) * 128)
                part = pgate[:, 0:128] * ts[0][:, sl]
                for e in range(1, local_exp):
                    part = part + pgate[:, e * 128:(e + 1) * 128] * ts[e][:, sl]
                acc[k, n * per + i, :, j * 128:(j + 1) * 128] = part

    mine = (c * 2 + y) * 2 * tok

    def core_copy(k, n):
        return remote(acc.at[k, n, pl.ds((1 - c) * 4 * tok, 4 * tok)], r_core.at[k, n], s_core.at[k, n], q_core.at[k, n], partner)

    def y_copy(k, n):
        return remote(acc.at[k, n, pl.ds((c * 2 + 1 - y) * 2 * tok, 2 * tok)], r_y.at[k, n], s_y.at[k, n], q_y.at[k, n], ypeer)

    def near_copy(n):
        return remote(acc.at[0, n, pl.ds(mine + (1 - zin) * tok, tok)], r_z.at[2, n], s_z.at[2, n], q_z.at[2, n], zpeer)

    def far_copy(j, n):
        return remote(acc.at[1, n, pl.ds(mine + j * tok, tok)], r_z.at[zin, n], s_z.at[j, n], q_z.at[zin, n], zfar[j])

    def far_wait(j, n):
        remote(acc.at[1, n, pl.ds(mine + j * tok, tok)], r_z.at[j, n], s_z.at[j, n], q_z.at[j, n], zfar[j]).wait_recv()

    def start_core(k, n):
        for i in range(per):
            core_copy(k, n * per + i).start()

    def after_core(k, m):
        for i in range(per):
            n = m * per + i
            core_copy(k, n).wait_recv()
            acc[k, n, pl.ds((c * 2 + 1 - y) * 2 * tok, 2 * tok)] += r_core[k, n, pl.ds((1 - y) * 2 * tok, 2 * tok)]
            y_copy(k, n).start()
            acc[k, n, pl.ds(mine, 2 * tok)] += r_core[k, n, pl.ds(y * 2 * tok, 2 * tok)]

    def after_y(k, n):
        y_copy(k, n).wait_recv()
        acc[k, n, pl.ds(mine, 2 * tok)] += r_y[k, n]
        if k == 0:
            near_copy(n).start()
        else:
            for j in range(2):
                far_copy(j, n).start()

    def finish(n):
        near_copy(n).wait_recv()
        for j in range(2):
            far_wait(j, n)
        cols = slice(n * cw, (n + 1) * cw)
        total = acc[0, n, pl.ds(mine + zin * tok, tok)] + r_z[2, n]
        total = total + (r_z[0, n] + r_z[1, n])
        out_ref[:, cols] = (x_ref[:, cols].astype(F32) + total).astype(BF16)

    finish_gather(pair)
    forward_far(0)
    route(pair)

    for e in range(local_exp):
        w_copy(e).wait()
        gate_up(e, pair)
        if e == 1:
            forward_far(1)
        if e == 3:
            forward_far_y(0)
    for i in range(local_exp, 2 * local_exp):
        w_copy(i).wait()

    def down0(n, _):
        down(n, 0)
        start_core(0, n)

        @pl.when(n > 0)
        def _():
            after_core(0, n - 1)

        @pl.when(n == 2)
        def _():
            forward_far_y(1)
        return 0
    lax.fori_loop(0, STEPS, down0, 0)

    finish_gather(1 - pair)
    route(1 - pair)
    for e in range(local_exp):
        gate_up(e, 1 - pair)
        if e == 0:
            after_core(0, STEPS - 1)
        if e % 2 == 1:
            for i in range(per):
                after_y(0, (e // 2) * per + i)

    def down1(n, _):
        down(n, 1)
        start_core(1, n)

        @pl.when(n > 0)
        def _():
            after_core(1, n - 1)

        @pl.when(n == 2)
        def _():
            for i in range(per):
                after_y(0, 2 * per + i)
        return 0
    lax.fori_loop(0, STEPS, down1, 0)
    after_core(1, STEPS - 1)
    for i in range(per):
        after_y(0, 3 * per + i)
    for n in range(PIECES):
        after_y(1, n)
    for n in range(PIECES):
        finish(n)

    sent(own, TO_Z, TO_Y, TO_C, TO_F0)

    @pl.when(is_mid)
    def _():
        sent(own, TO_F1)
        sent(near, TO_F0)
    for b in (near, *far):
        sent(b, TO_Y, TO_C)
    for b in (y_own, y_near, *y_far):
        sent(b, TO_C)
    for n in range(PIECES):
        for k in range(2):
            core_copy(k, n).wait_send()
            y_copy(k, n).wait_send()
            far_copy(k, n).wait_send()
        near_copy(n).wait_send()


def solution(mesh):
    n_group = mesh.shape['ep']
    rows_spec = P(('dp', 'ep'), None)

    def local_block(x_in, expert_ids, norm_weight, router_w, router_b, w_gate_up, b_gate_up, w_down, b_down):
        tok, d_model = x_in.shape
        top_k = expert_ids.shape[1]
        local_exp, d_ff = w_down.shape[0], w_down.shape[1]
        experts = local_exp * n_group
        cap = CAPACITY_FACTOR * top_k * tok // experts
        cfg = (tok, d_model, d_ff, top_k, experts, local_exp, cap)
        tc, ns, cw = 8 * tok, 8 * cap, d_model // PIECES
        vm = pl.BlockSpec(memory_space=pltpu.VMEM)
        hbm = pl.BlockSpec(memory_space=pl.ANY)
        dma = pltpu.SemaphoreType.DMA
        return pl.pallas_call(
            functools.partial(moe_kernel, cfg),
            out_shape=jax.ShapeDtypeStruct((tok, d_model), BF16),
            in_specs=[vm, vm, vm, vm, vm, hbm, vm, hbm, vm],
            out_specs=vm,
            scratch_shapes=[
                pltpu.VMEM((local_exp, d_model, 2 * d_ff), BF16),
                pltpu.VMEM((local_exp, d_ff, d_model), BF16),
                pltpu.VMEM((n_group * tok, d_model), BF16),
                pltpu.VMEM((n_group * tok // 2, 2 * experts), F32),
                pltpu.VMEM((local_exp * ns, tc), BF16),
                pltpu.VMEM((tc, local_exp * ns), BF16),
                pltpu.VMEM((tc, local_exp * 128), F32),
                pltpu.VMEM((128, tc), F32),
                pltpu.VMEM((ns, d_model), BF16),
                pltpu.VMEM((local_exp, ns, d_ff), BF16),
                pltpu.VMEM((256, 256), BF16),
                pltpu.VMEM((local_exp, 2 * d_ff), F32),
                pltpu.VMEM((local_exp, d_model), F32),
                pltpu.VMEM((2, PIECES, tc, cw), F32),
                pltpu.VMEM((2, PIECES, 4 * tok, cw), F32),
                pltpu.VMEM((2, PIECES, 2 * tok, cw), F32),
                pltpu.VMEM((3, PIECES, tok, cw), F32),
                dma((2 * local_exp,)),
                dma((5, n_group, 2)), dma((n_group, 2)), dma((5, n_group)), dma((n_group,)),
                dma((2, PIECES)), dma((2, PIECES)), dma((2, PIECES)), dma((2, PIECES)),
                dma((3, PIECES)), dma((3, PIECES)),
            ],
            compiler_params=pltpu.CompilerParams(
                collective_id=0, has_side_effects=True, vmem_limit_bytes=67043328),
            name='moe_block',
        )(x_in, expert_ids.T, norm_weight, router_w.T, router_b.reshape(1, -1), w_gate_up, b_gate_up, w_down, b_down)

    return jax.shard_map(local_block, mesh=mesh, in_specs=(rows_spec, rows_spec, P(), P(), P(), P('ep', None, None), P('ep', None), P('ep', None, None), P('ep', None)), out_specs=rows_spec, check_vma=False)
```

```python
import functools

import jax
import jax.numpy as jnp
from jax import lax
from jax.experimental import pallas as pl
from jax.experimental.pallas import tpu as pltpu
from jax.sharding import PartitionSpec as P

CAPACITY_FACTOR = 4
EPSILON = 1e-5
LIMIT = 7.0
ALPHA = 1.702
MESH = pl.DeviceIdType.MESH
PIECES = 4
STEPS = 4
F32 = jnp.float32
BF16 = jnp.bfloat16


def dot(a, b):
    return jnp.dot(a, b, preferred_element_type=F32)


def iota(shape, dim):
    return lax.broadcasted_iota(jnp.int32, shape, dim)


def moe_kernel(cfg, x_ref, ids_ref, g_ref, wr_ref, br_ref, wgu_hbm, bgu_ref, wd_hbm, bd_ref, out_ref,
               wgu, wd, hid, gate, sel, back, pgate, slot_t, rows, glu, perm, bgu, bd,
               acc, r_core, r_y, r_z,
               s_w, s_h, q_h, s_g, q_g, s_core, q_core, s_y, q_y, s_z, q_z):
    tok, d_model, d_ff, top_k, experts, local_exp, cap = cfg
    tc = 8 * tok
    ns = 8 * cap
    cw = d_model // PIECES
    half = tok // 2
    me = lax.axis_index('ep')
    z, y, c = lax.div(me, 4), lax.rem(lax.div(me, 2), 2), lax.rem(me, 2)
    pair, zin = lax.rem(z, 2), lax.div(z, 2)
    partner, ypeer, zpeer = me + 1 - 2 * c, me + 2 - 4 * y, me + 8 - 16 * zin
    zfar = [me + 4 * (2 * j + 1 - pair - z) for j in range(2)]
    is_mid = zin != pair

    def pos(q, cc, yy, zz):
        return ((q * 2 + cc) * 2 + yy) * 2 + zz

    def remote(src, dst, send, recv, dev):
        return pltpu.make_async_remote_copy(src_ref=src, dst_ref=dst, send_sem=send, recv_sem=recv,
                                            device_id={'ep': dev}, device_id_type=MESH)

    def w_copy(i):
        if i < local_exp:
            return pltpu.make_async_copy(wgu_hbm.at[i], wgu.at[i], s_w.at[i])
        return pltpu.make_async_copy(wd_hbm.at[i - local_exp], wd.at[i - local_exp], s_w.at[i])

    for i in range(2 * local_exp):
        w_copy(i).start()

    barrier = pltpu.get_barrier_semaphore()
    for dev in (partner, ypeer, zpeer, *zfar):
        pl.semaphore_signal(barrier, inc=1, device_id={'ep': dev}, device_id_type=MESH)

    own = pos(pair, c, y, zin)
    x = x_ref[...].astype(F32)
    inv = lax.rsqrt(jnp.mean(x * x, axis=-1, keepdims=True) + EPSILON)
    h = (x * inv * g_ref[...].reshape(1, d_model).astype(F32)).astype(BF16)
    hid[pl.ds(own * tok, tok), :] = h
    pl.semaphore_wait(barrier, 5)

    TO_Z, TO_Y, TO_C, TO_F0, TO_F1 = range(5)
    dest = [zpeer, ypeer, partner, me + 4 * (2 * zin + 1 - pair - z), me + 4 * (3 - 2 * zin - pair - z)]

    def h_copy(b, d, s):
        rs = pl.ds(b * tok + s * half, half)
        return remote(hid.at[rs], hid.at[rs], s_h.at[d, b, s], q_h.at[b, s], dest[d])

    def g_copy(b, d):
        rs = pl.ds(b * half, half)
        return remote(gate.at[rs], gate.at[rs], s_g.at[d, b], q_g.at[b], dest[d])

    def send_h(b, s, *ds):
        for d in ds:
            h_copy(b, d, s).start()

    def send_g(b, *ds):
        for d in ds:
            g_copy(b, d).start()

    def pass_h(b, s, *ds):
        h_copy(b, 0, s).wait_recv()
        send_h(b, s, *ds)

    def pass_g(b, *ds):
        g_copy(b, 0).wait_recv()
        send_g(b, *ds)

    def sent(b, *ds):
        for d in ds:
            for s in range(2):
                h_copy(b, d, s).wait_send()
            g_copy(b, d).wait_send()

    near = pos(pair, c, y, 1 - zin)
    y_own, y_near = pos(pair, c, 1 - y, zin), pos(pair, c, 1 - y, 1 - zin)
    far = [pos(1 - pair, c, y, j) for j in (zin, 1 - zin)]
    y_far = [pos(1 - pair, c, 1 - y, j) for j in (zin, 1 - zin)]

    for s in range(2):
        send_h(own, s, TO_Z, TO_Y)
    for s in range(2):
        send_h(own, s, TO_C)

    logits = lax.dot_general(h, wr_ref[...], (((1,), (1,)), ((), ())), preferred_element_type=F32) + br_ref[...].astype(F32)
    lane_e = iota((tok, experts), 1)
    ids = ids_ref[...].T
    chosen = ids[:, 0:1] == lane_e
    for k in range(1, top_k):
        chosen = jnp.logical_or(chosen, ids[:, k:k + 1] == lane_e)
    top = jnp.max(jnp.where(chosen, logits, -jnp.inf), axis=-1, keepdims=True)
    weight = jnp.where(chosen, jnp.exp(jnp.where(chosen, logits - top, 0.0)), 0.0)
    gates = jnp.where(chosen, weight / jnp.sum(weight, axis=-1, keepdims=True), -1.0)
    gate[pl.ds(own * half, half), :] = jnp.concatenate([gates[:half], gates[half:]], axis=1)
    send_g(own, TO_Z, TO_Y, TO_C, TO_F0)
    for s in range(2):
        send_h(own, s, TO_F0)

    @pl.when(is_mid)
    def _():
        send_g(own, TO_F1)
        for s in range(2):
            send_h(own, s, TO_F1)

    bgu[...] = bgu_ref[...].astype(F32)
    bd[...] = bd_ref[...].astype(F32)
    pi, pj = iota((256, 256), 0), iota((256, 256), 1)
    perm[...] = (lax.div(pi, 2) + 128 * lax.rem(pi, 2) == pj).astype(F32).astype(BF16)

    for s in range(2):
        pass_h(near, s, TO_Y, TO_C)
        pass_h(y_own, s, TO_C)
    pass_g(near, TO_Y, TO_C)
    pass_g(y_own, TO_C)

    @pl.when(is_mid)
    def _():
        send_g(near, TO_F0)
        for s in range(2):
            send_h(near, s, TO_F0)
    for s in range(2):
        pass_h(y_near, s, TO_C)
    pass_g(y_near, TO_C)

    def finish_gather(q):
        for yy in range(2):
            for zz in range(2):
                b = pos(q, 1 - c, yy, zz)
                for s in range(2):
                    pass_h(b, s)
                pass_g(b)

    def forward_far(j):
        pass_g(far[j], TO_Y, TO_C)
        for s in range(2):
            pass_h(far[j], s, TO_Y, TO_C)

    def forward_far_y(j):
        pass_g(y_far[j], TO_C)
        for s in range(2):
            pass_h(y_far[j], s, TO_C)

    def route(q):
        g2 = gate[pl.ds(q * 8 * half, 8 * half), :]
        g = jnp.concatenate([g2.reshape(8, half, 128), pltpu.roll(g2, experts, 1).reshape(8, half, 128)], axis=1).reshape(tc, 128)
        hit = g >= 0.0
        ri, rj = iota((tc, tc), 0), iota((tc, tc), 1)
        before = jnp.logical_and(rj < ri, lax.div(rj, tok) == lax.div(ri, tok)).astype(F32).astype(BF16)
        rank = dot(before, hit.astype(F32).astype(BF16))
        base = (lax.div(iota((tc, 128), 0), tok) * cap).astype(F32)
        slot = jnp.where(hit, rank + base, -1.0)
        slot_t[...] = slot.T
        lane = iota((tc, 128), 1)
        s_lane = iota((tc, ns), 1).astype(F32)
        s_row = iota((ns, tc), 0).astype(F32)
        for e in range(local_exp):
            col = me * local_exp + e
            pick = lane == col
            p_e = jnp.sum(jnp.where(pick, jnp.maximum(g, 0.0), 0.0), axis=1, keepdims=True)
            s_e = jnp.sum(jnp.where(pick, slot, 0.0), axis=1, keepdims=True)
            back[:, e * ns:(e + 1) * ns] = (s_e == s_lane).astype(F32).astype(BF16)
            pgate[:, e * 128:(e + 1) * 128] = jnp.broadcast_to(p_e, (tc, 128))
            sel[e * ns:(e + 1) * ns, :] = (slot_t[pl.ds(col, 1), :] == s_row).astype(F32).astype(BF16)

    def gate_up(e, q):
        pick = sel[e * ns:(e + 1) * ns, :]
        valid = jnp.max(pick.astype(F32), axis=1, keepdims=True) > 0.0
        rows[...] = dot(pick, hid[pl.ds(q * tc, tc), :]).astype(BF16)
        u = (dot(rows[...], wgu[e]) + bgu[e:e + 1, :]).astype(BF16)
        for j in range(2 * d_ff // 256):
            v = dot(u[:, j * 256:(j + 1) * 256], perm[...])
            a = jnp.minimum(v[:, :128], LIMIT)
            l = jnp.clip(v[:, 128:], -LIMIT, LIMIT)
            o = a * jax.nn.sigmoid(ALPHA * a) * (l + 1.0)
            glu[e, :, j * 128:(j + 1) * 128] = jnp.where(valid, o, 0.0).astype(BF16)

    per = PIECES // STEPS

    def down(n, k):
        cols = pl.ds(pl.multiple_of(n * (per * cw), 128), per * cw)
        ys = [(dot(glu[e], wd[e, :, cols]) + bd[e:e + 1, cols]).astype(BF16) for e in range(local_exp)]
        ts = [dot(back[:, e * ns:(e + 1) * ns], ys[e]) for e in range(local_exp)]
        for i in range(per):
            for j in range(cw // 128):
                sl = slice(i * cw + j * 128, i * cw + (j + 1) * 128)
                part = pgate[:, 0:128] * ts[0][:, sl]
                for e in range(1, local_exp):
                    part = part + pgate[:, e * 128:(e + 1) * 128] * ts[e][:, sl]
                acc[k, n * per + i, :, j * 128:(j + 1) * 128] = part

    mine = (c * 2 + y) * 2 * tok

    def core_copy(k, n):
        return remote(acc.at[k, n, pl.ds((1 - c) * 4 * tok, 4 * tok)], r_core.at[k, n], s_core.at[k, n], q_core.at[k, n], partner)

    def y_copy(k, n, j):
        return remote(acc.at[k, n, pl.ds(((c * 2 + 1 - y) * 2 + j) * tok, tok)], r_y.at[k, n, pl.ds(j * tok, tok)],
                      s_y.at[k, n, j], q_y.at[k, n, j], ypeer)

    def near_copy(n):
        return remote(acc.at[0, n, pl.ds(mine + (1 - zin) * tok, tok)], r_z.at[2, n], s_z.at[2, n], q_z.at[2, n], zpeer)

    def far_copy(j, n):
        return remote(acc.at[1, n, pl.ds(mine + j * tok, tok)], r_z.at[zin, n], s_z.at[j, n], q_z.at[zin, n], me + 4 * (2 * j + 1 - pair - z))

    def far_wait(j, n):
        remote(acc.at[1, n, pl.ds(mine + j * tok, tok)], r_z.at[j, n], s_z.at[j, n], q_z.at[j, n], zfar[j]).wait_recv()

    def start_core(k, n):
        for i in range(per):
            core_copy(k, n * per + i).start()

    def after_core(k, m):
        for i in range(per):
            n = m * per + i
            core_copy(k, n).wait_recv()
            acc[k, n, pl.ds((c * 2 + 1 - y) * 2 * tok, 2 * tok)] += r_core[k, n, pl.ds((1 - y) * 2 * tok, 2 * tok)]
            for j in (1 - zin, zin):
                y_copy(k, n, j).start()
            acc[k, n, pl.ds(mine, 2 * tok)] += r_core[k, n, pl.ds(y * 2 * tok, 2 * tok)]

    def after_y(k, n):
        for i, j in enumerate((1 - zin, zin)):
            y_copy(k, n, j).wait_recv()
            acc[k, n, pl.ds(mine + j * tok, tok)] += r_y[k, n, pl.ds(j * tok, tok)]
            if k == 1:
                far_copy(j, n).start()
            elif i == 0:
                near_copy(n).start()

    def finish(n):
        near_copy(n).wait_recv()
        for j in range(2):
            far_wait(j, n)
        cols = slice(n * cw, (n + 1) * cw)
        total = acc[0, n, pl.ds(mine + zin * tok, tok)] + r_z[2, n]
        total = total + (r_z[0, n] + r_z[1, n])
        out_ref[:, cols] = (x_ref[:, cols].astype(F32) + total).astype(BF16)

    finish_gather(pair)
    forward_far(0)
    route(pair)

    for e in range(local_exp):
        w_copy(e).wait()
        gate_up(e, pair)
        if e == 1:
            forward_far(1)
        if e == 3:
            forward_far_y(0)
    for i in range(local_exp, 2 * local_exp):
        w_copy(i).wait()

    def down0(n, _):
        down(n, 0)
        start_core(0, n)

        @pl.when(n > 0)
        def _():
            after_core(0, n - 1)

        @pl.when(n == 2)
        def _():
            forward_far_y(1)
        return 0
    lax.fori_loop(0, STEPS, down0, 0)

    finish_gather(1 - pair)
    route(1 - pair)
    for e in range(local_exp):
        gate_up(e, 1 - pair)
        if e == 0:
            after_core(0, STEPS - 1)
        if e % 2 == 1:
            for i in range(per):
                after_y(0, (e // 2) * per + i)

    def down1(n, _):
        down(n, 1)
        start_core(1, n)

        @pl.when(n > 0)
        def _():
            after_core(1, n - 1)

        @pl.when(n == 2)
        def _():
            for i in range(per):
                after_y(0, 2 * per + i)
        return 0
    lax.fori_loop(0, STEPS, down1, 0)
    after_core(1, STEPS - 1)
    for i in range(per):
        after_y(0, 3 * per + i)
    for n in range(PIECES):
        after_y(1, n)
    for n in range(PIECES):
        finish(n)

    sent(own, TO_Z, TO_Y, TO_C, TO_F0)

    @pl.when(is_mid)
    def _():
        sent(own, TO_F1)
        sent(near, TO_F0)
    for b in (near, *far):
        sent(b, TO_Y, TO_C)
    for b in (y_own, y_near, *y_far):
        sent(b, TO_C)
    for n in range(PIECES):
        for k in range(2):
            core_copy(k, n).wait_send()
            for j in range(2):
                y_copy(k, n, j).wait_send()
            far_copy(k, n).wait_send()
        near_copy(n).wait_send()


def solution(mesh):
    n_group = mesh.shape['ep']
    rows_spec = P(('dp', 'ep'), None)

    def local_block(x_in, expert_ids, norm_weight, router_w, router_b, w_gate_up, b_gate_up, w_down, b_down):
        tok, d_model = x_in.shape
        top_k = expert_ids.shape[1]
        local_exp, d_ff = w_down.shape[0], w_down.shape[1]
        experts = local_exp * n_group
        cap = CAPACITY_FACTOR * top_k * tok // experts
        cfg = (tok, d_model, d_ff, top_k, experts, local_exp, cap)
        tc, ns, cw = 8 * tok, 8 * cap, d_model // PIECES
        vm = pl.BlockSpec(memory_space=pltpu.VMEM)
        hbm = pl.BlockSpec(memory_space=pl.ANY)
        dma = pltpu.SemaphoreType.DMA
        return pl.pallas_call(
            functools.partial(moe_kernel, cfg),
            out_shape=jax.ShapeDtypeStruct((tok, d_model), BF16),
            in_specs=[vm, vm, vm, vm, vm, hbm, vm, hbm, vm],
            out_specs=vm,
            scratch_shapes=[
                pltpu.VMEM((local_exp, d_model, 2 * d_ff), BF16),
                pltpu.VMEM((local_exp, d_ff, d_model), BF16),
                pltpu.VMEM((n_group * tok, d_model), BF16),
                pltpu.VMEM((n_group * tok // 2, 2 * experts), F32),
                pltpu.VMEM((local_exp * ns, tc), BF16),
                pltpu.VMEM((tc, local_exp * ns), BF16),
                pltpu.VMEM((tc, local_exp * 128), F32),
                pltpu.VMEM((128, tc), F32),
                pltpu.VMEM((ns, d_model), BF16),
                pltpu.VMEM((local_exp, ns, d_ff), BF16),
                pltpu.VMEM((256, 256), BF16),
                pltpu.VMEM((local_exp, 2 * d_ff), F32),
                pltpu.VMEM((local_exp, d_model), F32),
                pltpu.VMEM((2, PIECES, tc, cw), F32),
                pltpu.VMEM((2, PIECES, 4 * tok, cw), F32),
                pltpu.VMEM((2, PIECES, 2 * tok, cw), F32),
                pltpu.VMEM((3, PIECES, tok, cw), F32),
                dma((2 * local_exp,)),
                dma((5, n_group, 2)), dma((n_group, 2)), dma((5, n_group)), dma((n_group,)),
                dma((2, PIECES)), dma((2, PIECES)), dma((2, PIECES, 2)), dma((2, PIECES, 2)),
                dma((3, PIECES)), dma((3, PIECES)),
            ],
            compiler_params=pltpu.CompilerParams(
                collective_id=0, has_side_effects=True, vmem_limit_bytes=67043328),
            name='moe_block',
        )(x_in, expert_ids.T, norm_weight, router_w.T, router_b.reshape(1, -1), w_gate_up, b_gate_up, w_down, b_down)

    return jax.shard_map(local_block, mesh=mesh, in_specs=(rows_spec, rows_spec, P(), P(), P(), P('ep', None, None), P('ep', None), P('ep', None, None), P('ep', None)), out_specs=rows_spec, check_vma=False)
```
